32 devices in a mesh: dp: 8 (over y, x, core), mp: 4 (over z).
Axes of the slice: x: 2, y: 2, z: 4, core: 2. Of those that a mesh axis runs over, the one named last changes fastest.
Arguments:
- inputs: bfloat16 [1568, 16, 1024], P('mp', 'dp'), may hold values from -6 to 6
- teacher: bfloat16 [1568, 16, 1024], P('mp', 'dp'), may hold values from -6 to 6
- clip_tokens: int32 [16], P('dp'), may hold values from 1 to 1568, 18816 in all
- owners: int32 [192], replicated, may hold values from 0 to 7, as said below
- qkv_master: float32 [8, 128, 3, 1024], P(None, 'dp', None, 'mp'), may hold values from -0.1875 to 0.1875
- out_master: float32 [8, 128, 1024], P('mp', 'dp'), may hold values from -3 to 3
- up_master: float32 [8, 128, 4096], P(None, 'dp', 'mp'), may hold values from -0.1875 to 0.1875
- down_master: float32 [32, 128, 1024], P('mp', 'dp'), may hold values from -0.09375 to 0.09375
- norm_gains: float32 [2, 1024], replicated, may hold values from 0.25 to 1.75
- shift_vectors: float32 [4, 1024], replicated, may hold values from -0.8 to 0.8
- split_vectors: float32 [4, 1536], P('mp'), may hold values from -1.2 to 1.2
- bases: float32 [384, 4, 2, 128, 128], P('dp', 'mp'), may hold values from -1 to 1, as said below
- first_moments: float32 [384, 4, 128, 128], P('dp', 'mp'), may hold values from -5 to 5
- second_moments: float32 [384, 4, 128, 128], P('dp', 'mp'), may hold values from 0.2 to 2
- plain_first: float32 [6, 1024], replicated, may hold values from -5 to 5
- plain_second: float32 [6, 1024], replicated, may hold values from 0.2 to 2
- split_first: float32 [4, 1536], P('mp'), may hold values from -5 to 5
- split_second: float32 [4, 1536], P('mp'), may hold values from 0.2 to 2
Outputs:
- output: bfloat16 [1568, 16, 1024], P('mp', 'dp')
- input_grad: float32 [1568, 16, 1024], P('mp', 'dp')
- qkv_new: float32 [8, 128, 3, 1024], P(None, 'dp', None, 'mp')
- out_new: float32 [8, 128, 1024], P('mp', 'dp')
- up_new: float32 [8, 128, 4096], P(None, 'dp', 'mp')
- down_new: float32 [32, 128, 1024], P('mp', 'dp')
- qkv_copy: bfloat16 [8, 128, 3, 1024], P(None, 'dp', None, 'mp')
- out_copy: bfloat16 [8, 128, 1024], P('mp', 'dp')
- up_copy: bfloat16 [8, 128, 4096], P(None, 'dp', 'mp')
- down_copy: bfloat16 [32, 128, 1024], P('mp', 'dp')
- gains_new: float32 [2, 1024], replicated
- shifts_new: float32 [4, 1024], replicated
- split_new: float32 [4, 1536], P('mp')
- first_new: float32 [384, 4, 128, 128], P('dp', 'mp')
- second_new: float32 [384, 4, 128, 128], P('dp', 'mp')
- plain_first_new: float32 [6, 1024], replicated
- plain_second_new: float32 [6, 1024], replicated
- split_first_new: float32 [4, 1536], P('mp')
- split_second_new: float32 [4, 1536], P('mp')
The draws below stay inside these ranges and needn't reach their ends.
Inputs may be any that keep to these rules, and one draw needn't show every extreme that they name: `owners`: no dp index owns more than 48 blocks; one index owns exactly 48. bases[m, g, 0] and bases[m, g, 1] are orthogonal to float32 rounding.
All inputs are finite; a program needn't handle non-finite values. No bound on the sum of `clip_tokens` on one device may be relied on, other than what follows from the above.
Results may differ from the reference program's by a relative error of at most 0.013.
Values may be sent and summed in bfloat16 or wider, within the bound.
A program may use at most 384 MiB of HBM per device.

```python
import math
import jax
import jax.numpy as jnp
import numpy as np
from jax import lax

D = 1024
FF = 4096
HD = 64
SEQ = 1568
B = 128
CLIPS = 16
NBLK = 192
CAP = 48
SLOTS = 384
VS = 1536
N_DP = 8
N_MP = 4


def draw_owners(key, part):
    key_top, key_slots, key_order = jax.random.split(key, 3)
    busiest = jax.random.randint(key_top, (), 0, N_DP)
    chosen = jax.random.permutation(key_slots, (N_DP - 1) * CAP)[:NBLK - CAP]
    other_owner = chosen // CAP
    other_owner = other_owner + (other_owner >= busiest).astype(jnp.int32)
    owner_list = jnp.concatenate([jnp.full((CAP,), busiest, jnp.int32), other_owner.astype(jnp.int32)])
    return jax.random.permutation(key_order, owner_list).astype(jnp.int32)


def draw_split_vectors(key, part):
    group_width = D // N_MP
    column_count = 2 * group_width + FF // N_MP
    noise_rows = jnp.clip(jax.random.normal(key, (N_MP, column_count), jnp.float32), -4.0, 4.0)
    columns = jnp.arange(column_count)
    spread = jnp.where(columns < 2 * group_width, 0.05, 0.3)
    return noise_rows * spread[None, :]


def draw_bases(key, part):
    total_count = SLOTS * N_MP * 2
    basis_keys = jax.random.split(key, total_count)
    indices = jnp.arange(B, dtype=jnp.int32)
    common_bits = indices[:, None] & indices[None, :]
    parity = jnp.zeros((B, B), jnp.int32)
    for bit_number in range(B.bit_length()):
        parity = parity + (common_bits >> bit_number & 1)
    hadamard = (1.0 - 2.0 * (parity % 2).astype(jnp.float32)) / math.sqrt(B)

    def one_basis(basis_key):
        key_perm, key_sign, key_angle = jax.random.split(basis_key, 3)
        row_order = jax.random.permutation(key_perm, B)
        row_signs = 1.0 - 2.0 * jax.random.randint(key_sign, (B,), 0, 2).astype(jnp.float32)
        signed_rows = row_signs[:, None] * hadamard[row_order, :]
        angles = jax.random.uniform(key_angle, (B // 2,), jnp.float32, -math.pi, math.pi)
        cosines = jnp.cos(angles)
        sines = jnp.sin(angles)
        col_pairs = signed_rows.reshape(B, B // 2, 2)
        left_col = cosines * col_pairs[:, :, 0] - sines * col_pairs[:, :, 1]
        right_col = sines * col_pairs[:, :, 0] + cosines * col_pairs[:, :, 1]
        return jnp.stack([left_col, right_col], axis=-1).reshape(B, B)
    return jax.vmap(one_basis)(basis_keys).reshape(SLOTS, N_MP, 2, B, B)


def level_of(stream_key, dims, cuts, smallest, high):
    gain = 1.0
    for axis_at, shards_of in cuts:
        steps = jax.random.uniform(jax.random.fold_in(jax.random.fold_in(stream_key, 6), axis_at), (shards_of,), jnp.float32, smallest / len(cuts), high / len(cuts))
        gain = gain * jnp.repeat(jnp.exp(steps), dims[axis_at] // shards_of).reshape((-1,) + (1,) * (len(dims) - 1 - axis_at))
    return gain


def profile(count, total, bound, slope):
    weights = [(1 << 20) // math.isqrt(grade ** slope) + 1 for grade in range(2, count + 1)]
    rest, given = total - bound - (count - 1), [1] * (count - 1)
    while rest > 0:
        candidates = [i for i in range(count - 1) if given[i] < bound]
        pool, left = sum([weights[i] for i in candidates]), rest
        for i in candidates:
            extra = min(bound - given[i], max(1, left * weights[i] // pool), rest)
            given[i] = given[i] + extra
            rest = rest - extra
    return np.array([bound] + given)


def uneven(stream_key, number_of, total, most, slope):
    if number_of == 2:
        one = jax.random.randint(stream_key, (), max(1, total - most), min(most, total - 1) + 1)
        return jnp.stack([one, total - one])
    lengths = jnp.asarray(profile(number_of, total, most, slope), jnp.int32)
    twos = (number_of - 1) // 2
    giver, sink = lengths[1:1 + 2 * twos:2], lengths[2:2 + 2 * twos:2]
    room = jnp.minimum(giver - 1, most - sink)
    passed = jax.random.randint(jax.random.fold_in(stream_key, 1), (twos,), 0, 1 << 20) % (room + 1)
    lengths = lengths.at[1:1 + 2 * twos:2].set(giver - passed).at[2:2 + 2 * twos:2].set(sink + passed)
    return lengths[jax.random.permutation(jax.random.fold_in(stream_key, 2), number_of)]


def gaussian(stream_key, dims, deviation, reach, cuts=(), held_as=jnp.bfloat16):
    level = level_of(stream_key, dims, cuts, -0.22, 0.18) if cuts else 1.0
    array = jax.random.normal(stream_key, dims, jnp.float32) * deviation * level
    return jnp.minimum(jnp.maximum(array, -reach), reach).astype(held_as)


def setup_inputs(seed: int = 0) -> dict:
    streams_of = jax.random.split(jax.random.key(seed), 19)
    return {
        "inputs": gaussian(streams_of[0], (SEQ, CLIPS, D), 1.0, 6.0, ((0, 4), (1, 8))),
        "teacher": gaussian(streams_of[1], (SEQ, CLIPS, D), 1.0, 6.0, ((0, 4), (1, 8))),
        "clip_tokens": uneven(streams_of[2], CLIPS, CLIPS * SEQ * 3 // 4, SEQ, 1).astype(jnp.int32),
        "owners": draw_owners(jax.random.fold_in(streams_of[18], 71), 0),
        "qkv_master": gaussian(streams_of[4], (D // B, B, 3, D), D ** -0.5, 0.1875, ((1, 8), (3, 4)), jnp.float32),
        "out_master": gaussian(streams_of[5], (D // B, B, D), 4 ** -0.5, 3.0, ((0, 4), (1, 8)), jnp.float32),
        "up_master": gaussian(streams_of[6], (D // B, B, FF), D ** -0.5, 0.1875, ((1, 8), (2, 4)), jnp.float32),
        "down_master": gaussian(streams_of[7], (FF // B, B, D), FF ** -0.5, 0.09375, ((0, 4), (1, 8)), jnp.float32),
        "norm_gains": jnp.clip(1.0 + 0.15 * jax.random.normal(streams_of[8], (2, D), jnp.float32), 0.25, 1.75),
        "shift_vectors": gaussian(streams_of[9], (4, D), 0.2, 0.8, (), jnp.float32),
        "split_vectors": draw_split_vectors(jax.random.fold_in(streams_of[18], 71), 0),
        "bases": draw_bases(jax.random.fold_in(streams_of[18], 71), 0),
        "first_moments": gaussian(streams_of[12], (SLOTS, N_MP, B, B), 1.0, 5.0, ((0, 8), (1, 4)), jnp.float32),
        "second_moments": jnp.clip(jnp.exp(math.log(2.0) - 2.3025851 * jax.random.uniform(streams_of[13], (SLOTS, N_MP, B, B), jnp.float32) ** level_of(streams_of[13], (SLOTS, N_MP, B, B), ((0, 8), (1, 4)), -0.2, 0.2)), 0.2, 2.0),
        "plain_first": gaussian(streams_of[14], (6, D), 1.0, 5.0, (), jnp.float32),
        "plain_second": jnp.clip(jnp.exp(jax.random.uniform(streams_of[15], (6, D), jnp.float32, math.log(0.2), math.log(2.0))), 0.2, 2.0),
        "split_first": gaussian(streams_of[16], (N_MP, VS), 1.0, 5.0, ((0, 4),), jnp.float32),
        "split_second": jnp.clip(jnp.exp(math.log(2.0) - 2.3025851 * jax.random.uniform(streams_of[17], (N_MP, VS), jnp.float32) ** level_of(streams_of[17], (N_MP, VS), ((0, 4),), -0.2, 0.2)), 0.2, 2.0),
    }


@jax.custom_vjp
def low(v):
    return lax.optimization_barrier(v.astype(jnp.bfloat16)).astype(jnp.float32)

@jax.custom_vjp
def low_back(v):
    return v

def low_keep(v):
    return (low(v), None)

def low_pass(kept, grad):
    return (grad,)

def back_keep(v):
    return (v, None)

def back_low(kept, grad):
    return (low(grad),)
low.defvjp(low_keep, low_pass)
low_back.defvjp(back_keep, back_low)
eps_norm = 1e-06
eps_adam = 1e-08
beta_first = 0.5
beta_second = 0.6
rate_qkv = 0.016
rate_out = 0.25
rate_up = 0.016
rate_down = 0.008
rate_vector = 0.3
scale_score = 0.125
highest = lax.Precision.HIGHEST

def layer_norm(values, scale_row, shift_row):
    average = lax.optimization_barrier(jnp.mean(values, axis=-1, keepdims=True))
    centered = values - average
    variance = lax.optimization_barrier(jnp.mean(centered * centered, axis=-1, keepdims=True))
    return centered * lax.rsqrt(variance + 1e-06) * scale_row + shift_row

def adam_rows(grad_rows, param_rows, first_rows, second_rows):
    scaled = grad_rows * lax.rsqrt(lax.optimization_barrier(jnp.mean(grad_rows * grad_rows, axis=-1, keepdims=True)) + eps_norm)
    new_first = beta_first * first_rows + (1.0 - beta_first) * scaled
    new_second = beta_second * second_rows + (1.0 - beta_second) * scaled * scaled
    step_rows = new_first / (jnp.sqrt(new_second) + eps_adam)
    return (param_rows - rate_vector * step_rows, new_first, new_second)

def rotate_adam(grad_blocks, left_basis, right_basis, old_first, old_second):
    scaled = grad_blocks * lax.rsqrt(lax.optimization_barrier(jnp.mean(grad_blocks * grad_blocks, axis=(1, 2), keepdims=True)) + eps_norm)
    rotated = jnp.einsum('kba,kbd->kad', left_basis, scaled, precision=highest)
    rotated = jnp.einsum('kad,kde->kae', rotated, right_basis, precision=highest)
    new_first = beta_first * old_first + (1.0 - beta_first) * rotated
    new_second = beta_second * old_second + (1.0 - beta_second) * rotated * rotated
    step_rot = new_first / (jnp.sqrt(new_second) + eps_adam)
    update = jnp.einsum('kab,kbd->kad', left_basis, step_rot, precision=highest)
    update = jnp.einsum('kad,ked->kae', update, right_basis, precision=highest)
    return (new_first, new_second, update)

def clip_layer(weights, tokens, length):
    qkv_weight, out_weight, up_weight, down_weight, gain_rows, shift_rows, split_rows = weights
    group_width = D // N_MP
    head_count = D // HD
    seq_len = tokens.shape[0]
    query_bias = split_rows[:, :group_width].reshape(D)
    value_bias = split_rows[:, group_width:2 * group_width].reshape(D)
    up_bias = split_rows[:, 2 * group_width:].reshape(FF)
    normed = low(layer_norm(tokens, gain_rows[0], shift_rows[0]))
    projected = jnp.dot(normed, qkv_weight, precision=highest)
    full_bias = jnp.concatenate([query_bias, jnp.zeros((D,), jnp.float32), value_bias])
    projected = low(low_back(projected + full_bias))
    queries = projected[:, :D].reshape(seq_len, head_count, HD)
    key_rows = projected[:, D:2 * D].reshape(seq_len, head_count, HD)
    value_rows = projected[:, 2 * D:].reshape(seq_len, head_count, HD)
    scores = low_back(jnp.einsum('qhe,khe->hqk', queries, key_rows, precision=highest) * scale_score)
    key_valid = jnp.arange(seq_len) < length
    scores = jnp.where(key_valid[None, None, :], scores, -1e+30)
    row_top = lax.optimization_barrier(jnp.max(scores, axis=-1, keepdims=True))
    exponent = jnp.exp(scores - row_top)
    probability = low(exponent / lax.optimization_barrier(jnp.sum(exponent, axis=-1, keepdims=True)))
    attended = jnp.einsum('hqk,khe->qhe', probability, value_rows, precision=highest).reshape(seq_len, D)
    attended = low(low_back(attended))
    hidden = tokens + low_back(jnp.dot(attended, out_weight, precision=highest)) + shift_rows[1]
    normed_two = low(layer_norm(hidden, gain_rows[1], shift_rows[2]))
    upper_pre = low_back(jnp.dot(normed_two, up_weight, precision=highest) + up_bias)
    active = low(jax.nn.gelu(upper_pre, approximate=False))
    return hidden + low_back(jnp.dot(active, down_weight, precision=highest)) + shift_rows[3]

def reference(inputs, teacher, clip_tokens, owners, qkv_master, out_master, up_master, down_master, norm_gains, shift_vectors, split_vectors, bases, first_moments, second_moments, plain_first, plain_second, split_first, split_second):
    masters = (qkv_master, out_master, up_master, down_master, norm_gains, shift_vectors, split_vectors)

    def forward(params, tokens):
        qkv_param, out_param, up_param, down_param, gain_rows, shift_rows, split_rows = params
        weights = (low(qkv_param).reshape(D, 3 * D), low(out_param).reshape(D, D), low(up_param).reshape(D, FF), low(down_param).reshape(FF, D), gain_rows, shift_rows, split_rows)

        def one_clip(pair):
            return clip_layer(weights, pair[0], pair[1])
        per_clip = lax.map(jax.checkpoint(one_clip), (jnp.moveaxis(tokens, 1, 0), clip_tokens))
        return jnp.moveaxis(per_clip, 0, 1)
    tokens32 = inputs.astype(jnp.float32)
    final_rows, pull_back = jax.vjp(forward, masters, tokens32)
    row_valid = jnp.arange(SEQ)[:, None] < clip_tokens[None, :]
    cotangent = jnp.where(row_valid[:, :, None], final_rows - teacher.astype(jnp.float32), 0.0)
    grad_params, input_grad = pull_back(cotangent)
    grad_qkv, grad_out, grad_up, grad_down, grad_gains, grad_shifts, grad_split = grad_params
    block_ids = jnp.arange(NBLK)
    same_owner = owners[:, None] == owners[None, :]
    earlier = block_ids[None, :] < block_ids[:, None]
    slot_pos = lax.optimization_barrier(jnp.sum((same_owner & earlier).astype(jnp.int32), axis=1))
    slots = owners * CAP + slot_pos
    group_width = D // N_MP
    group_ff = FF // N_MP
    full_qkv = grad_qkv.reshape(D, 3, D)
    full_out = grad_out.reshape(D, D)
    full_up = grad_up.reshape(D, FF)
    full_down = grad_down.reshape(FF, D)
    count_qkv = D // B * 3 * (group_width // B)
    count_out = group_width // B * (D // B)
    count_up = D // B * (group_ff // B)
    first_out = first_moments
    second_out = second_moments
    qkv_parts, out_parts, up_parts, down_parts = ([], [], [], [])
    for group_index in range(N_MP):
        low_col = group_index * group_width
        low_ff = group_index * group_ff
        qkv_blocks = full_qkv[:, :, low_col:low_col + group_width].reshape(D // B, B, 3, group_width // B, B).transpose(0, 2, 3, 1, 4).reshape(-1, B, B)
        out_blocks = full_out[low_col:low_col + group_width].reshape(group_width // B, B, D // B, B).transpose(0, 2, 1, 3).reshape(-1, B, B)
        up_blocks = full_up[:, low_ff:low_ff + group_ff].reshape(D // B, B, group_ff // B, B).transpose(0, 2, 1, 3).reshape(-1, B, B)
        down_blocks = full_down[low_ff:low_ff + group_ff].reshape(group_ff // B, B, D // B, B).transpose(0, 2, 1, 3).reshape(-1, B, B)
        grad_blocks = jnp.concatenate([qkv_blocks, out_blocks, up_blocks, down_blocks], axis=0)
        left_basis = bases[slots, group_index, 0]
        right_basis = bases[slots, group_index, 1]
        new_first, new_second, update = rotate_adam(grad_blocks, left_basis, right_basis, first_moments[slots, group_index], second_moments[slots, group_index])
        first_out = first_out.at[slots, group_index].set(new_first)
        second_out = second_out.at[slots, group_index].set(new_second)
        qkv_parts.append(update[:count_qkv].reshape(D // B, 3, group_width // B, B, B).transpose(0, 3, 1, 2, 4).reshape(D, 3, group_width))
        out_parts.append(update[count_qkv:count_qkv + count_out].reshape(group_width // B, D // B, B, B).transpose(0, 2, 1, 3).reshape(group_width, D))
        up_parts.append(update[count_qkv + count_out:count_qkv + count_out + count_up].reshape(D // B, group_ff // B, B, B).transpose(0, 2, 1, 3).reshape(D, group_ff))
        down_parts.append(update[count_qkv + count_out + count_up:].reshape(group_ff // B, D // B, B, B).transpose(0, 2, 1, 3).reshape(group_ff, D))
    qkv_new = qkv_master - rate_qkv * jnp.concatenate(qkv_parts, axis=2).reshape(D // B, B, 3, D)
    out_new = out_master - rate_out * jnp.concatenate(out_parts, axis=0).reshape(D // B, B, D)
    up_new = up_master - rate_up * jnp.concatenate(up_parts, axis=1).reshape(D // B, B, FF)
    down_new = down_master - rate_down * jnp.concatenate(down_parts, axis=0).reshape(FF // B, B, D)
    plain_grad = jnp.stack([grad_gains[0], grad_shifts[0], grad_shifts[1], grad_gains[1], grad_shifts[2], grad_shifts[3]])
    plain_param = jnp.stack([norm_gains[0], shift_vectors[0], shift_vectors[1], norm_gains[1], shift_vectors[2], shift_vectors[3]])
    plain_new, plain_first_new, plain_second_new = adam_rows(plain_grad, plain_param, plain_first, plain_second)
    gains_new = jnp.stack([plain_new[0], plain_new[3]])
    shifts_new = jnp.stack([plain_new[1], plain_new[2], plain_new[4], plain_new[5]])
    split_new, split_first_new, split_second_new = adam_rows(grad_split, split_vectors, split_first, split_second)
    return (final_rows.astype(jnp.bfloat16), input_grad, qkv_new, out_new, up_new, down_new, qkv_new.astype(jnp.bfloat16), out_new.astype(jnp.bfloat16), up_new.astype(jnp.bfloat16), down_new.astype(jnp.bfloat16), gains_new, shifts_new, split_new, first_out, second_out, plain_first_new, plain_second_new, split_first_new, split_second_new)
```

```python
from functools import partial

import jax
import jax.numpy as jnp
from jax import lax
from jax.experimental import pallas as pl
from jax.experimental.pallas import tpu as pltpu
from jax.sharding import PartitionSpec as P

HD = 64
B = 128
PAIR = 2 * HD


eps_norm = 1e-06
eps_adam = 1e-08
beta_first = 0.5
beta_second = 0.6
rate_qkv = 0.016
rate_out = 0.25
rate_up = 0.016
rate_down = 0.008
rate_vector = 0.3
scale_score = 0.125

f32 = jnp.float32
bf16 = jnp.bfloat16
NT = (((1,), (1,)), ((), ()))
NN = (((1,), (0,)), ((), ()))
TN = (((0,), (0,)), ((), ()))


def dot(left, right, dims=NN):
    return lax.dot_general(left, right, dims, preferred_element_type=f32)


def layer_norm(values, scale_row, shift_row):
    average = jnp.mean(values, axis=-1, keepdims=True)
    centered = values - average
    variance = jnp.mean(centered * centered, axis=-1, keepdims=True)
    return centered * lax.rsqrt(variance + 1e-06) * scale_row + shift_row


def adam_rows(grad_rows, param_rows, first_rows, second_rows):
    scaled = grad_rows * lax.rsqrt(
        jnp.mean(grad_rows * grad_rows, axis=-1, keepdims=True) + eps_norm
    )
    new_first = beta_first * first_rows + (1.0 - beta_first) * scaled
    new_second = beta_second * second_rows + (1.0 - beta_second) * scaled * scaled
    step_rows = new_first / (jnp.sqrt(new_second) + eps_adam)
    return (param_rows - rate_vector * step_rows, new_first, new_second)


def rotate_adam(grad_blocks, left_basis, right_basis, old_first, old_second):
    high = lax.Precision.HIGH
    scaled = grad_blocks * lax.rsqrt(
        jnp.mean(grad_blocks * grad_blocks, axis=(1, 2), keepdims=True) + eps_norm
    )
    rotated = jnp.einsum("kba,kbd->kad", left_basis, scaled, precision=high)
    rotated = jnp.einsum("kad,kde->kae", rotated, right_basis, precision=high)
    new_first = beta_first * old_first + (1.0 - beta_first) * rotated
    new_second = beta_second * old_second + (1.0 - beta_second) * rotated * rotated
    step_rot = new_first / (jnp.sqrt(new_second) + eps_adam)
    update = jnp.einsum("kab,kbd->kad", left_basis, step_rot, precision=high)
    update = jnp.einsum("kad,ked->kae", update, right_basis, precision=high)
    return (new_first, new_second, update)


def lane_index(rows):
    return lax.broadcasted_iota(jnp.int32, (rows, PAIR), 1)


def own_lanes(lane, head):
    return lane < HD if head == 0 else lane >= HD


def key_operands(keys, first_row, valid):
    rows = keys.shape[0]
    lane = lane_index(rows)
    row = lax.broadcasted_iota(jnp.int32, (rows, PAIR), 0) + first_row
    wide = keys.astype(f32)
    padding = jnp.where(row >= valid, -1e30, 0.0)
    operands = []
    for head in range(2):
        base = HD * (1 - head)
        other = jnp.where(lane < base + 3, 1.0, jnp.where(lane == base + 3, padding, 0.0))
        operands.append(jnp.where(own_lanes(lane, head), wide, other).astype(bf16))
    return operands


def forward_kernel(chunk, valid_ref, q_ref, k_ref, v_ref, out_ref, log_ref, key_ref, score_ref):
    tokens = q_ref.shape[0]
    lane = lane_index(tokens)
    queries = q_ref[...].astype(f32) * scale_score
    ones = jnp.ones((16, chunk), f32)
    starts = range(0, tokens, chunk)
    outputs, logs = [], []
    for head, operand in enumerate(key_operands(k_ref[...], 0, valid_ref[0])):
        mark = jnp.where(lane == HD * (1 - head) + 3, 1.0, 0.0)
        query = jnp.where(own_lanes(lane, head), queries, mark).astype(bf16)
        key_ref[head] = operand
        top = None
        for at in starts:
            scores = dot(key_ref[head, at : at + chunk], query, NT)
            score_ref[head, at : at + chunk] = scores
            peak = jnp.max(scores, axis=0, keepdims=True)
            top = peak if top is None else jnp.maximum(top, peak)
        total = None
        for at in starts:
            turned = jnp.transpose(v_ref[at : at + chunk].astype(f32))
            values = jnp.concatenate([turned[HD * head : HD * head + HD], ones], axis=0)
            weight = jnp.exp(score_ref[head, at : at + chunk] - top).astype(bf16)
            term = dot(values.astype(bf16), weight)
            total = term if total is None else total + term
        weight_sum = total[HD : HD + 1]
        outputs.append(total[:HD] / weight_sum)
        logs.append(-(top + jnp.log(weight_sum)))
    out_ref[...] = jnp.transpose(jnp.concatenate(outputs, axis=0)).astype(bf16)
    column = jnp.ones((HD, 1), f32)
    log_ref[...] = jnp.transpose(jnp.concatenate([column * logs[1], column * logs[0]], axis=0))


def attend_forward(proj, valid, first_pair, pairs, chunk):
    tokens = proj.shape[0]
    per_part = proj.shape[1] // 3 // PAIR

    def pair_spec(at):
        return pl.BlockSpec((tokens, PAIR), lambda pair: (0, at + pair))

    return pl.pallas_call(
        partial(forward_kernel, chunk),
        grid=(pairs,),
        in_specs=[
            pl.BlockSpec(memory_space=pltpu.SMEM),
            pair_spec(first_pair),
            pair_spec(per_part + first_pair),
            pair_spec(2 * per_part + first_pair),
        ],
        out_specs=[pair_spec(0), pair_spec(0)],
        out_shape=[
            jax.ShapeDtypeStruct((tokens, pairs * PAIR), bf16),
            jax.ShapeDtypeStruct((tokens, pairs * PAIR), f32),
        ],
        scratch_shapes=[
            pltpu.VMEM((2, tokens, PAIR), bf16),
            pltpu.VMEM((2, tokens, tokens), f32),
        ],
        compiler_params=pltpu.CompilerParams(
            dimension_semantics=("arbitrary",), vmem_limit_bytes=58 * 2**20
        ),
        cost_estimate=pl.CostEstimate(
            flops=16 * pairs * tokens * tokens * PAIR,
            bytes_accessed=pairs * tokens * PAIR * 12,
            transcendentals=pairs * 2 * tokens * tokens,
        ),
    )(valid, proj, proj, proj)


def backward_kernel(
    valid_ref,
    q_ref,
    k_ref,
    v_ref,
    grad_ref,
    out_ref,
    log_ref,
    dq_ref,
    dk_ref,
    dv_ref,
    query_ref,
    cot_ref,
    turned_ref,
):
    step = pl.program_id(1)
    rows = k_ref.shape[0]
    lane = lane_index(q_ref.shape[0])

    @pl.when(step == 0)
    def _():
        queries = q_ref[...].astype(f32) * scale_score
        logs = log_ref[...]
        log_high = logs.astype(bf16).astype(f32)
        log_rest = logs - log_high
        log_middle = log_rest.astype(bf16).astype(f32)
        log_low = log_rest - log_middle
        grad = grad_ref[...].astype(f32)
        product = grad * out_ref[...].astype(f32)
        product_high = product.astype(bf16)
        product_low = (product - product_high.astype(f32)).astype(bf16)
        source = lax.broadcasted_iota(jnp.int32, (PAIR, PAIR), 0)
        target = lax.broadcasted_iota(jnp.int32, (PAIR, PAIR), 1)
        place = jnp.where((source < HD) != (target < HD), -1.0, 0.0).astype(bf16)
        delta = dot(product_high, place) + dot(product_low, place)
        delta_high = delta.astype(bf16).astype(f32)
        delta_low = delta - delta_high
        for head in range(2):
            base = HD * (1 - head)
            mine = own_lanes(lane, head)
            mark = jnp.where(lane == base + 3, 1.0, 0.0)
            other = jnp.where(lane == base + 2, log_low, mark)
            other = jnp.where(lane == base + 1, log_middle, other)
            other = jnp.where(lane == base, log_high, other)
            query_ref[head] = jnp.where(mine, queries, other).astype(bf16)
            other = jnp.where(lane == base + 1, delta_low, 0.0)
            other = jnp.where(lane == base, delta_high, other)
            cot_ref[head] = jnp.where(mine, grad, other).astype(bf16)
        turned_ref[...] = jnp.zeros_like(turned_ref)

    operands = key_operands(k_ref[...], step * rows, valid_ref[0])
    key_lane = lane_index(rows)
    wide_values = v_ref[...].astype(f32)
    turned_keys = jnp.transpose(k_ref[...].astype(f32)).astype(bf16)
    dk, dv = [], []
    for head in range(2):
        base = HD * (1 - head)
        span = slice(HD * head, HD * head + HD)
        pair_of_ones = jnp.where((key_lane == base) | (key_lane == base + 1), 1.0, 0.0)
        values = jnp.where(own_lanes(key_lane, head), wide_values, pair_of_ones).astype(bf16)
        weight = jnp.exp(dot(operands[head], query_ref[head], NT))
        slope = (weight * dot(values, cot_ref[head], NT)).astype(bf16)
        dv.append(dot(weight.astype(bf16), cot_ref[head]))
        dk.append(dot(slope, query_ref[head]))
        turned_ref[span] += dot(turned_keys[span], slope)
    dk_ref[...] = jnp.where(key_lane < HD, dk[0], dk[1]).astype(bf16)
    dv_ref[...] = jnp.where(key_lane < HD, dv[0], dv[1]).astype(bf16)

    @pl.when(step == pl.num_programs(1) - 1)
    def _():
        dq_ref[...] = (jnp.transpose(turned_ref[...]) * scale_score).astype(bf16)


def attend_backward(proj, grad, attended, logs, valid, first_pair, pairs, row_block):
    tokens = proj.shape[0]
    per_part = proj.shape[1] // 3 // PAIR

    def whole(at):
        return pl.BlockSpec((tokens, PAIR), lambda pair, step: (0, at + pair))

    def block(at):
        return pl.BlockSpec((row_block, PAIR), lambda pair, step: (step, at + pair))

    return pl.pallas_call(
        backward_kernel,
        grid=(pairs, tokens // row_block),
        in_specs=[
            pl.BlockSpec(memory_space=pltpu.SMEM),
            whole(first_pair),
            block(per_part + first_pair),
            block(2 * per_part + first_pair),
            whole(0),
            whole(0),
            whole(0),
        ],
        out_specs=[whole(0), block(0), block(0)],
        out_shape=[jax.ShapeDtypeStruct((tokens, pairs * PAIR), bf16)] * 3,
        scratch_shapes=[
            pltpu.VMEM((2, tokens, PAIR), bf16),
            pltpu.VMEM((2, tokens, PAIR), bf16),
            pltpu.VMEM((PAIR, tokens), f32),
        ],
        compiler_params=pltpu.CompilerParams(
            dimension_semantics=("arbitrary", "arbitrary"), vmem_limit_bytes=58 * 2**20
        ),
        cost_estimate=pl.CostEstimate(
            flops=40 * pairs * tokens * tokens * PAIR,
            bytes_accessed=pairs * tokens * PAIR * 24,
            transcendentals=pairs * 2 * tokens * tokens,
        ),
    )(valid, proj, proj, proj, grad, attended, logs)


def exchange(values, axis):
    return lax.all_to_all(values, axis, split_axis=0, concat_axis=0, tiled=True)


def sum_everywhere(values):
    for axis in ("dp", "mp"):
        size = lax.axis_size(axis)
        bit = 1
        while bit < size:
            values = values + lax.ppermute(values, axis, [(i, i ^ bit) for i in range(size)])
            bit *= 2
    return values


def per_device(
    inputs,
    teacher,
    clip_tokens,
    owners,
    qkv_master,
    out_master,
    up_master,
    down_master,
    norm_gains,
    shift_vectors,
    split_vectors,
    bases,
    first_moments,
    second_moments,
    plain_first,
    plain_second,
    split_first,
    split_second,
):
    local_rows, clips_here, width = inputs.shape
    groups = lax.axis_size("mp")
    group_index = lax.axis_index("mp")
    shard_count = lax.axis_size("dp")
    shard_index = lax.axis_index("dp")
    seq_len = local_rows * groups
    row_blocks, shard_rows, _, group_width = qkv_master.shape
    group_ff = up_master.shape[2]
    ff = group_ff * groups
    tokens_here = clips_here * local_rows
    parts = groups // clips_here
    part_groups = groups // parts
    part_width = part_groups * group_width
    my_clip = group_index // parts
    my_part = group_index % parts
    pairs = part_width // PAIR
    calls = 2
    call_pairs = pairs // calls
    call_width = call_pairs * PAIR
    row_block = seq_len // 7

    positions = group_index * local_rows + jnp.arange(local_rows)
    row_valid = positions[None, :] < clip_tokens[:, None]
    valid = lax.dynamic_slice(clip_tokens, (my_clip,), (1,))

    split_all = lax.all_gather(split_vectors[0], "mp", axis=0)
    qkv_groups = lax.all_gather(
        qkv_master.astype(bf16).reshape(row_blocks, shard_rows, 3 * group_width), "mp", axis=0
    )
    qkv_part = lax.dynamic_slice_in_dim(qkv_groups, my_part * part_groups, part_groups, axis=0)
    qkv_part = (
        qkv_part.reshape(part_groups, row_blocks, shard_rows, 3, group_width)
        .transpose(1, 2, 3, 0, 4)
        .reshape(row_blocks, shard_rows, 3 * part_width)
    )
    qkv_weight = lax.all_gather(qkv_part, "dp", axis=1, tiled=True).reshape(width, 3 * part_width)

    def both_axes(master, mp_axis):
        over_mp = lax.all_gather(master.astype(bf16), "mp", axis=mp_axis, tiled=True)
        return lax.all_gather(over_mp, "dp", axis=1, tiled=True)

    out_weight = both_axes(out_master, 0).reshape(width, width)
    up_weight = both_axes(up_master, 2).reshape(width, ff)
    down_weight = both_axes(down_master, 0).reshape(ff, width)
    part_bias = lax.dynamic_slice_in_dim(
        split_all[:, : 2 * group_width].reshape(groups, 2, group_width),
        my_part * part_groups,
        part_groups,
        axis=0,
    ).transpose(1, 0, 2).reshape(2, part_width)
    up_bias = split_all[:, 2 * group_width :].reshape(ff)

    tokens = inputs.transpose(1, 0, 2).astype(f32)
    normed = layer_norm(tokens, norm_gains[0], shift_vectors[0]).astype(bf16)
    normed_clip = exchange(jnp.repeat(normed, parts, axis=0), "mp").reshape(seq_len, width)
    proj_bias = jnp.concatenate([part_bias[0], jnp.zeros_like(part_bias[0]), part_bias[1]])
    proj = (dot(normed_clip, qkv_weight) + proj_bias).astype(bf16)
    attended_parts, log_parts, received = [], [], []
    for call in range(calls):
        attended_call, logs_call = attend_forward(
            proj, valid, call * call_pairs, call_pairs, row_block
        )
        attended_parts.append(attended_call)
        log_parts.append(logs_call)
        received.append(exchange(attended_call.reshape(groups, local_rows, call_width), "mp"))
    attended = (
        jnp.stack(received)
        .reshape(calls, clips_here, parts, local_rows, call_width)
        .transpose(1, 3, 2, 0, 4)
        .reshape(tokens_here, width)
    )
    tokens = tokens.reshape(tokens_here, width)
    hidden = tokens + dot(attended, out_weight) + shift_vectors[1]
    normed_two = layer_norm(hidden, norm_gains[1], shift_vectors[2]).astype(bf16)
    upper = dot(normed_two, up_weight) + up_bias
    gelu = partial(jax.nn.gelu, approximate=False)
    active, gelu_pull = jax.vjp(gelu, upper)
    active = active.astype(bf16)
    final = hidden + dot(active, down_weight) + shift_vectors[3]
    output = final.astype(bf16).reshape(clips_here, local_rows, width).transpose(1, 0, 2)

    target = teacher.transpose(1, 0, 2).reshape(tokens_here, width).astype(f32)
    grad_final = jnp.where(row_valid.reshape(tokens_here, 1), final - target, 0.0)
    grad_final_low = grad_final.astype(bf16)
    grad_active = dot(grad_final_low, down_weight, NT)
    grad_upper = gelu_pull(grad_active)[0].astype(bf16)
    grad_normed_two = dot(grad_upper, up_weight, NT)
    _, norm_two_pull = jax.vjp(layer_norm, hidden, norm_gains[1], shift_vectors[2])
    hidden_part, grad_gain_two, grad_shift_two = norm_two_pull(grad_normed_two)
    grad_hidden = grad_final + hidden_part
    grad_hidden_low = grad_hidden.astype(bf16)
    grad_attended = dot(grad_hidden_low, out_weight, NT).astype(bf16)
    outgoing_grad = (
        grad_attended.reshape(clips_here, local_rows, parts, calls, call_width)
        .transpose(3, 0, 2, 1, 4)
        .reshape(calls, groups, local_rows, call_width)
    )
    grad_parts = [
        exchange(outgoing_grad[call], "mp").reshape(seq_len, call_width) for call in range(calls)
    ]

    def scatter_rows(grad, shape):
        return lax.psum_scatter(
            grad.astype(bf16).reshape(shape), "dp", scatter_dimension=1, tiled=True
        )

    grad_down = scatter_rows(dot(active, grad_final_low, TN), (ff // B, B, width))
    grad_up = scatter_rows(dot(normed_two, grad_upper, TN), (row_blocks, B, ff))
    grad_out = scatter_rows(dot(attended, grad_hidden_low, TN), (width // B, B, width))
    early = jnp.concatenate(
        [
            jnp.sum(grad_hidden, axis=0),
            grad_gain_two,
            grad_shift_two,
            jnp.sum(grad_final, axis=0),
            jnp.sum(grad_upper, axis=0, dtype=f32),
        ]
    )
    early_total = sum_everywhere(early.reshape(-1, width))
    by_group = jnp.concatenate(
        [
            grad_out.reshape(groups, -1, shard_rows, width),
            grad_up.reshape(row_blocks, shard_rows, groups, group_ff).transpose(2, 0, 1, 3),
            grad_down.reshape(groups, -1, shard_rows, width),
        ],
        axis=1,
    )
    own = jnp.sum(
        exchange(by_group, "mp").reshape(groups, -1, shard_rows, width).astype(f32), axis=0
    )
    count = group_width // B
    out_shard, up_shard, down_shard = own[:count], own[count : count + row_blocks], own[count + row_blocks :]

    pieces = []
    for call in range(calls):
        pieces.append(
            attend_backward(
                proj,
                grad_parts[call],
                attended_parts[call],
                log_parts[call],
                valid,
                call * call_pairs,
                call_pairs,
                row_block,
            )
        )
    grad_proj = jnp.concatenate([piece[kind] for kind in range(3) for piece in pieces], axis=1)
    grad_normed_part = dot(grad_proj, qkv_weight, NT).astype(bf16)
    grad_qkv = scatter_rows(
        dot(normed_clip, grad_proj, TN), (row_blocks, B, 3 * part_width)
    )
    returned_grad = exchange(grad_normed_part.reshape(groups, local_rows, width), "mp")
    grad_normed = jnp.sum(
        returned_grad.reshape(clips_here, parts, local_rows, width).astype(f32), axis=1
    ).reshape(tokens_here, width)
    _, norm_one_pull = jax.vjp(layer_norm, tokens, norm_gains[0], shift_vectors[0])
    tokens_part, grad_gain_one, grad_shift_one = norm_one_pull(grad_normed)
    input_grad = (
        (grad_hidden + tokens_part).reshape(clips_here, local_rows, width).transpose(1, 0, 2)
    )
    part_sums = jnp.sum(grad_proj, axis=0, dtype=f32).reshape(3, part_width)
    placed_sums = jnp.where(
        jnp.arange(parts)[:, None, None] == my_part, part_sums[None, ::2], 0.0
    )
    bias_rows = placed_sums.transpose(1, 0, 2).reshape(2, width)
    late = jnp.concatenate([grad_gain_one[None], grad_shift_one[None], bias_rows])
    late_total = sum_everywhere(late)
    plain_total = jnp.concatenate([late_total[:2], early_total[:4]])
    split_grad = jnp.concatenate(
        [
            late_total[2].reshape(groups, group_width),
            late_total[3].reshape(groups, group_width),
            early_total[4:].reshape(groups, group_ff),
        ],
        axis=1,
    )
    split_total = lax.dynamic_slice_in_dim(split_grad, group_index, 1, axis=0)

    qkv_groups_grad = (
        grad_qkv.reshape(row_blocks, shard_rows, 3, part_groups, group_width)
        .transpose(3, 0, 1, 2, 4)
        .reshape(1, part_groups, row_blocks, shard_rows, 3 * group_width)
    )
    here = jnp.arange(parts)[:, None, None, None, None] == my_part
    qkv_sent = jnp.where(here, qkv_groups_grad, jnp.zeros((), bf16)).reshape(
        groups, row_blocks, shard_rows, 3 * group_width
    )
    qkv_shard = jnp.sum(
        exchange(qkv_sent, "mp").astype(f32), axis=0
    ).reshape(row_blocks, shard_rows, 3, group_width)

    grad_blocks = jnp.concatenate(
        [
            qkv_shard.reshape(row_blocks, shard_rows, 3, group_width // B, B)
            .transpose(0, 2, 3, 1, 4)
            .reshape(-1, shard_rows, B),
            out_shard.reshape(group_width // B, shard_rows, row_blocks, B)
            .transpose(0, 2, 1, 3)
            .reshape(-1, shard_rows, B),
            up_shard.reshape(row_blocks, shard_rows, group_ff // B, B)
            .transpose(0, 2, 1, 3)
            .reshape(-1, shard_rows, B),
            down_shard.reshape(group_ff // B, shard_rows, row_blocks, B)
            .transpose(0, 2, 1, 3)
            .reshape(-1, shard_rows, B),
        ],
        axis=0,
    ).astype(bf16)
    cap_count = bases.shape[0]
    block_ids = jnp.arange(owners.shape[0])
    same_owner = owners[:, None] == owners[None, :]
    earlier = block_ids[None, :] < block_ids[:, None]
    slot_pos = jnp.sum((same_owner & earlier).astype(jnp.int32), axis=1)
    select = (
        (slot_pos[None, None, :] == jnp.arange(cap_count)[:, None, None])
        & (owners[None, None, :] == jnp.arange(shard_count)[None, :, None])
    ).astype(bf16)
    outgoing = jnp.einsum("cjk,krb->cjrb", select, grad_blocks, preferred_element_type=bf16)
    incoming = (
        lax.all_to_all(outgoing, "dp", split_axis=1, concat_axis=1, tiled=True)
        .astype(f32)
        .reshape(cap_count, B, B)
    )
    slot_used = jnp.any(
        (owners[None, :] == shard_index) & (slot_pos[None, :] == jnp.arange(cap_count)[:, None]),
        axis=1,
    )
    old_first = first_moments[:, 0]
    old_second = second_moments[:, 0]
    new_first, new_second, update = rotate_adam(
        incoming, bases[:, 0, 0], bases[:, 0, 1], old_first, old_second
    )
    first_new = jnp.where(slot_used[:, None, None], new_first, old_first)[:, None]
    second_new = jnp.where(slot_used[:, None, None], new_second, old_second)[:, None]
    returned = lax.all_to_all(
        update.reshape(cap_count, shard_count, shard_rows, B).astype(bf16),
        "dp",
        split_axis=1,
        concat_axis=1,
        tiled=True,
    )
    picked = jnp.take(
        returned.reshape(cap_count * shard_count, shard_rows, B),
        slot_pos * shard_count + owners,
        axis=0,
    ).astype(f32)
    count_qkv = row_blocks * 3 * (group_width // B)
    count_out = group_width // B * row_blocks
    count_up = row_blocks * (group_ff // B)
    qkv_update = (
        picked[:count_qkv]
        .reshape(row_blocks, 3, group_width // B, shard_rows, B)
        .transpose(0, 3, 1, 2, 4)
        .reshape(row_blocks, shard_rows, 3, group_width)
    )
    out_update = (
        picked[count_qkv : count_qkv + count_out]
        .reshape(group_width // B, row_blocks, shard_rows, B)
        .transpose(0, 2, 1, 3)
        .reshape(group_width // B, shard_rows, width)
    )
    up_update = (
        picked[count_qkv + count_out : count_qkv + count_out + count_up]
        .reshape(row_blocks, group_ff // B, shard_rows, B)
        .transpose(0, 2, 1, 3)
        .reshape(row_blocks, shard_rows, group_ff)
    )
    down_update = (
        picked[count_qkv + count_out + count_up :]
        .reshape(group_ff // B, row_blocks, shard_rows, B)
        .transpose(0, 2, 1, 3)
        .reshape(group_ff // B, shard_rows, width)
    )
    qkv_new = qkv_master - rate_qkv * qkv_update
    out_new = out_master - rate_out * out_update
    up_new = up_master - rate_up * up_update
    down_new = down_master - rate_down * down_update
    plain_param = jnp.stack(
        [
            norm_gains[0],
            shift_vectors[0],
            shift_vectors[1],
            norm_gains[1],
            shift_vectors[2],
            shift_vectors[3],
        ]
    )
    plain_new, plain_first_new, plain_second_new = adam_rows(
        plain_total, plain_param, plain_first, plain_second
    )
    gains_new = jnp.stack([plain_new[0], plain_new[3]])
    shifts_new = jnp.stack([plain_new[1], plain_new[2], plain_new[4], plain_new[5]])
    split_new, split_first_new, split_second_new = adam_rows(
        split_total, split_vectors, split_first, split_second
    )
    return (
        output,
        input_grad,
        qkv_new,
        out_new,
        up_new,
        down_new,
        qkv_new.astype(bf16),
        out_new.astype(bf16),
        up_new.astype(bf16),
        down_new.astype(bf16),
        gains_new,
        shifts_new,
        split_new,
        first_new,
        second_new,
        plain_first_new,
        plain_second_new,
        split_first_new,
        split_second_new,
    )


def solution(mesh):
    placed = (
        P("mp", "dp", None),
        P("mp", "dp", None),
        P("dp"),
        P(),
        P(None, "dp", None, "mp"),
        P("mp", "dp", None),
        P(None, "dp", "mp"),
        P("mp", "dp", None),
        P(),
        P(),
        P("mp", None),
        P("dp", "mp", None, None, None),
        P("dp", "mp", None, None),
        P("dp", "mp", None, None),
        P(),
        P(),
        P("mp", None),
        P("mp", None),
    )
    return jax.shard_map(
        per_device,
        mesh=mesh,
        in_specs=placed,
        out_specs=(
            P("mp", "dp", None),
            P("mp", "dp", None),
            P(None, "dp", None, "mp"),
            P("mp", "dp", None),
            P(None, "dp", "mp"),
            P("mp", "dp", None),
            P(None, "dp", None, "mp"),
            P("mp", "dp", None),
            P(None, "dp", "mp"),
            P("mp", "dp", None),
            P(),
            P(),
            P("mp", None),
            P("dp", "mp", None, None),
            P("dp", "mp", None, None),
            P(),
            P(),
            P("mp", None),
            P("mp", None),
        ),
        check_vma=False,
    )
```

```python
from functools import partial

import jax
import jax.numpy as jnp
from jax import lax
from jax.experimental import pallas as pl
from jax.experimental.pallas import tpu as pltpu
from jax.sharding import PartitionSpec as P


HD = 64
B = 128
PAIR = 2 * HD


eps_norm = 1e-06
eps_adam = 1e-08
beta_first = 0.5
beta_second = 0.6
rate_qkv = 0.016
rate_out = 0.25
rate_up = 0.016
rate_down = 0.008
rate_vector = 0.3
scale_score = 0.125

f32 = jnp.float32
bf16 = jnp.bfloat16
NT = (((1,), (1,)), ((), ()))
NN = (((1,), (0,)), ((), ()))
TN = (((0,), (0,)), ((), ()))


def dot(left, right, dims=NN):
    return lax.dot_general(left, right, dims, preferred_element_type=f32)


def layer_norm(values, scale_row, shift_row):
    average = jnp.mean(values, axis=-1, keepdims=True)
    centered = values - average
    variance = jnp.mean(centered * centered, axis=-1, keepdims=True)
    return centered * lax.rsqrt(variance + 1e-06) * scale_row + shift_row


def adam_rows(grad_rows, param_rows, first_rows, second_rows):
    scaled = grad_rows * lax.rsqrt(
        jnp.mean(grad_rows * grad_rows, axis=-1, keepdims=True) + eps_norm
    )
    new_first = beta_first * first_rows + (1.0 - beta_first) * scaled
    new_second = beta_second * second_rows + (1.0 - beta_second) * scaled * scaled
    step_rows = new_first / (jnp.sqrt(new_second) + eps_adam)
    return (param_rows - rate_vector * step_rows, new_first, new_second)


def rotate_adam(grad_blocks, left_basis, right_basis, old_first, old_second):
    high = lax.Precision.HIGH
    scaled = grad_blocks * lax.rsqrt(
        jnp.mean(grad_blocks * grad_blocks, axis=(1, 2), keepdims=True) + eps_norm
    )
    rotated = jnp.einsum("kba,kbd->kad", left_basis, scaled, precision=high)
    rotated = jnp.einsum("kad,kde->kae", rotated, right_basis, precision=high)
    new_first = beta_first * old_first + (1.0 - beta_first) * rotated
    new_second = beta_second * old_second + (1.0 - beta_second) * rotated * rotated
    step_rot = new_first / (jnp.sqrt(new_second) + eps_adam)
    update = jnp.einsum("kab,kbd->kad", left_basis, step_rot, precision=high)
    update = jnp.einsum("kad,ked->kae", update, right_basis, precision=high)
    return (new_first, new_second, update)


def lane_index(rows):
    return lax.broadcasted_iota(jnp.int32, (rows, PAIR), 1)


def own_lanes(lane, head):
    return lane < HD if head == 0 else lane >= HD


def key_operands(keys, first_row, valid):
    rows = keys.shape[0]
    lane = lane_index(rows)
    row = lax.broadcasted_iota(jnp.int32, (rows, PAIR), 0) + first_row
    wide = keys.astype(f32)
    padding = jnp.where(row >= valid, -1e30, 0.0)
    operands = []
    for head in range(2):
        base = HD * (1 - head)
        other = jnp.where(lane < base + 3, 1.0, jnp.where(lane == base + 3, padding, 0.0))
        operands.append(jnp.where(own_lanes(lane, head), wide, other).astype(bf16))
    return operands


def forward_kernel(chunk, valid_ref, q_ref, k_ref, v_ref, out_ref, log_ref, key_ref, score_ref):
    tokens = q_ref.shape[0]
    lane = lane_index(tokens)
    queries = q_ref[...].astype(f32) * scale_score
    ones = jnp.ones((16, chunk), f32)
    starts = range(0, tokens, chunk)
    outputs, logs = [], []
    for head, operand in enumerate(key_operands(k_ref[...], 0, valid_ref[0])):
        mark = jnp.where(lane == HD * (1 - head) + 3, 1.0, 0.0)
        query = jnp.where(own_lanes(lane, head), queries, mark).astype(bf16)
        key_ref[head] = operand
        top = None
        for at in starts:
            scores = dot(key_ref[head, at : at + chunk], query, NT)
            score_ref[head, at : at + chunk] = scores
            peak = jnp.max(scores, axis=0, keepdims=True)
            top = peak if top is None else jnp.maximum(top, peak)
        total = None
        for at in starts:
            turned = jnp.transpose(v_ref[at : at + chunk].astype(f32))
            values = jnp.concatenate([turned[HD * head : HD * head + HD], ones], axis=0)
            weight = jnp.exp(score_ref[head, at : at + chunk] - top).astype(bf16)
            term = dot(values.astype(bf16), weight)
            total = term if total is None else total + term
        weight_sum = total[HD : HD + 1]
        outputs.append(total[:HD] / weight_sum)
        logs.append(-(top + jnp.log(weight_sum)))
    out_ref[...] = jnp.transpose(jnp.concatenate(outputs, axis=0)).astype(bf16)
    column = jnp.ones((HD, 1), f32)
    log_ref[...] = jnp.transpose(jnp.concatenate([column * logs[1], column * logs[0]], axis=0))


def attend_forward(proj, valid, first_pair, pairs, chunk):
    tokens = proj.shape[0]
    per_part = proj.shape[1] // 3 // PAIR

    def pair_spec(at):
        return pl.BlockSpec((tokens, PAIR), lambda pair: (0, at + pair))

    return pl.pallas_call(
        partial(forward_kernel, chunk),
        grid=(pairs,),
        in_specs=[
            pl.BlockSpec(memory_space=pltpu.SMEM),
            pair_spec(first_pair),
            pair_spec(per_part + first_pair),
            pair_spec(2 * per_part + first_pair),
        ],
        out_specs=[pair_spec(0), pair_spec(0)],
        out_shape=[
            jax.ShapeDtypeStruct((tokens, pairs * PAIR), bf16),
            jax.ShapeDtypeStruct((tokens, pairs * PAIR), f32),
        ],
        scratch_shapes=[
            pltpu.VMEM((2, tokens, PAIR), bf16),
            pltpu.VMEM((2, tokens, tokens), f32),
        ],
        compiler_params=pltpu.CompilerParams(
            dimension_semantics=("arbitrary",), vmem_limit_bytes=58 * 2**20
        ),
        cost_estimate=pl.CostEstimate(
            flops=16 * pairs * tokens * tokens * PAIR,
            bytes_accessed=pairs * tokens * PAIR * 12,
            transcendentals=pairs * 2 * tokens * tokens,
        ),
    )(valid, proj, proj, proj)


def backward_kernel(
    valid_ref,
    q_ref,
    k_ref,
    v_ref,
    grad_ref,
    out_ref,
    log_ref,
    dq_ref,
    dk_ref,
    dv_ref,
    query_ref,
    cot_ref,
    turned_ref,
):
    step = pl.program_id(1)
    rows = k_ref.shape[0]
    lane = lane_index(q_ref.shape[0])

    @pl.when(step == 0)
    def _():
        queries = q_ref[...].astype(f32) * scale_score
        logs = log_ref[...]
        log_high = logs.astype(bf16).astype(f32)
        log_rest = logs - log_high
        log_middle = log_rest.astype(bf16).astype(f32)
        log_low = log_rest - log_middle
        grad = grad_ref[...].astype(f32)
        product = grad * out_ref[...].astype(f32)
        product_high = product.astype(bf16)
        product_low = (product - product_high.astype(f32)).astype(bf16)
        source = lax.broadcasted_iota(jnp.int32, (PAIR, PAIR), 0)
        target = lax.broadcasted_iota(jnp.int32, (PAIR, PAIR), 1)
        place = jnp.where((source < HD) != (target < HD), -1.0, 0.0).astype(bf16)
        delta = dot(product_high, place) + dot(product_low, place)
        delta_high = delta.astype(bf16).astype(f32)
        delta_low = delta - delta_high
        for head in range(2):
            base = HD * (1 - head)
            mine = own_lanes(lane, head)
            mark = jnp.where(lane == base + 3, 1.0, 0.0)
            other = jnp.where(lane == base + 2, log_low, mark)
            other = jnp.where(lane == base + 1, log_middle, other)
            other = jnp.where(lane == base, log_high, other)
            query_ref[head] = jnp.where(mine, queries, other).astype(bf16)
            other = jnp.where(lane == base + 1, delta_low, 0.0)
            other = jnp.where(lane == base, delta_high, other)
            cot_ref[head] = jnp.where(mine, grad, other).astype(bf16)
        turned_ref[...] = jnp.zeros_like(turned_ref)

    operands = key_operands(k_ref[...], step * rows, valid_ref[0])
    key_lane = lane_index(rows)
    wide_values = v_ref[...].astype(f32)
    turned_keys = jnp.transpose(k_ref[...].astype(f32)).astype(bf16)
    dk, dv = [], []
    for head in range(2):
        base = HD * (1 - head)
        span = slice(HD * head, HD * head + HD)
        pair_of_ones = jnp.where((key_lane == base) | (key_lane == base + 1), 1.0, 0.0)
        values = jnp.where(own_lanes(key_lane, head), wide_values, pair_of_ones).astype(bf16)
        weight = jnp.exp(dot(operands[head], query_ref[head], NT))
        slope = (weight * dot(values, cot_ref[head], NT)).astype(bf16)
        dv.append(dot(weight.astype(bf16), cot_ref[head]))
        dk.append(dot(slope, query_ref[head]))
        turned_ref[span] += dot(turned_keys[span], slope)
    dk_ref[...] = jnp.where(key_lane < HD, dk[0], dk[1]).astype(bf16)
    dv_ref[...] = jnp.where(key_lane < HD, dv[0], dv[1]).astype(bf16)

    @pl.when(step == pl.num_programs(1) - 1)
    def _():
        dq_ref[...] = (jnp.transpose(turned_ref[...]) * scale_score).astype(bf16)


def attend_backward(proj, grad, attended, logs, valid, first_pair, pairs, row_block):
    tokens = proj.shape[0]
    per_part = proj.shape[1] // 3 // PAIR

    def whole(at):
        return pl.BlockSpec((tokens, PAIR), lambda pair, step: (0, at + pair))

    def block(at):
        return pl.BlockSpec((row_block, PAIR), lambda pair, step: (step, at + pair))

    return pl.pallas_call(
        backward_kernel,
        grid=(pairs, tokens // row_block),
        in_specs=[
            pl.BlockSpec(memory_space=pltpu.SMEM),
            whole(first_pair),
            block(per_part + first_pair),
            block(2 * per_part + first_pair),
            whole(0),
            whole(0),
            whole(0),
        ],
        out_specs=[whole(0), block(0), block(0)],
        out_shape=[jax.ShapeDtypeStruct((tokens, pairs * PAIR), bf16)] * 3,
        scratch_shapes=[
            pltpu.VMEM((2, tokens, PAIR), bf16),
            pltpu.VMEM((2, tokens, PAIR), bf16),
            pltpu.VMEM((PAIR, tokens), f32),
        ],
        compiler_params=pltpu.CompilerParams(
            dimension_semantics=("arbitrary", "arbitrary"), vmem_limit_bytes=58 * 2**20
        ),
        cost_estimate=pl.CostEstimate(
            flops=40 * pairs * tokens * tokens * PAIR,
            bytes_accessed=pairs * tokens * PAIR * 24,
            transcendentals=pairs * 2 * tokens * tokens,
        ),
    )(valid, proj, proj, proj, grad, attended, logs)


def feed_kernel(chunk, normed_ref, weight_ref, bias_ref, active_ref, slope_ref):
    for at in range(0, normed_ref.shape[0], chunk):
        rows = slice(at, at + chunk)
        upper = dot(normed_ref[rows], weight_ref[...]) + bias_ref[...]
        below = 0.5 + 0.5 * lax.erf(upper * 0.7071067811865476)
        active_ref[rows] = (upper * below).astype(bf16)
        density = 0.3989422804014327 * jnp.exp(-0.5 * upper * upper)
        slope_ref[rows] = (below + upper * density).astype(bf16)


def feed_up(normed, weight, bias):
    tokens, width = normed.shape
    columns = 512
    by_column = pl.BlockSpec((tokens, columns), lambda step: (0, step))
    return pl.pallas_call(
        partial(feed_kernel, tokens // 7),
        grid=(weight.shape[1] // columns,),
        in_specs=[
            pl.BlockSpec((tokens, width), lambda step: (0, 0)),
            pl.BlockSpec((width, columns), lambda step: (0, step)),
            pl.BlockSpec((1, columns), lambda step: (0, step)),
        ],
        out_specs=[by_column, by_column],
        out_shape=[jax.ShapeDtypeStruct((tokens, weight.shape[1]), bf16)] * 2,
        compiler_params=pltpu.CompilerParams(
            dimension_semantics=("arbitrary",), vmem_limit_bytes=48 * 2**20
        ),
        cost_estimate=pl.CostEstimate(
            flops=2 * tokens * width * weight.shape[1],
            bytes_accessed=4 * tokens * weight.shape[1] + 2 * width * weight.shape[1],
            transcendentals=2 * tokens * weight.shape[1],
        ),
    )(normed, weight, bias)


def exchange(values, axis):
    return lax.all_to_all(values, axis, split_axis=0, concat_axis=0, tiled=True)


def gather(values, axis, dimension):
    return lax.all_gather(values, axis, axis=dimension, tiled=True)


def scatter(values):
    return lax.psum_scatter(values, "dp", scatter_dimension=1, tiled=True)


def send_steps(pieces, axis):
    size = lax.axis_size(axis)
    arrived = [pieces[0]]
    for step in range(1, size):
        arrived.append(lax.ppermute(pieces[step], axis, [(i, i ^ step) for i in range(size)]))
    return arrived


def send_all(values, axis):
    size = lax.axis_size(axis)
    arrived = [values]
    for step in range(1, size):
        arrived.append(lax.ppermute(values, axis, [(i, i ^ step) for i in range(size)]))
    return jnp.concatenate(arrived, axis=0)


def sum_pieces(pieces, axis):
    total = None
    for piece in send_steps(pieces, axis):
        total = piece.astype(f32) if total is None else total + piece.astype(f32)
    return total


def sum_everywhere(values):
    for axis in ("dp", "mp"):
        size = lax.axis_size(axis)
        bit = 1
        while bit < size:
            other = lax.ppermute(values, axis, [(i, i ^ bit) for i in range(size)])
            values = values + other
            bit *= 2
    return values


def per_device(
    inputs,
    teacher,
    clip_tokens,
    owners,
    qkv_master,
    out_master,
    up_master,
    down_master,
    norm_gains,
    shift_vectors,
    split_vectors,
    bases,
    first_moments,
    second_moments,
    plain_first,
    plain_second,
    split_first,
    split_second,
):
    local_rows, clips_here, width = inputs.shape
    groups = lax.axis_size("mp")
    group_index = lax.axis_index("mp")
    shard_count = lax.axis_size("dp")
    shard_index = lax.axis_index("dp")
    seq_len = local_rows * groups
    row_blocks, shard_rows, _, group_width = qkv_master.shape
    group_ff = up_master.shape[2]
    ff = group_ff * groups
    tokens_here = clips_here * local_rows
    assert groups == 4 and clips_here == 2
    parts = groups // clips_here
    part_groups = groups // parts
    part_width = part_groups * group_width
    my_clip = group_index // parts
    my_part = group_index % parts
    pairs = part_width // PAIR
    calls = 2
    call_pairs = pairs // calls
    call_width = call_pairs * PAIR
    row_block = seq_len // 7

    positions = group_index * local_rows + jnp.arange(local_rows)
    row_valid = positions[None, :] < clip_tokens[:, None]
    valid = lax.dynamic_slice(clip_tokens, (my_clip,), (1,))
    near_order = group_index ^ jnp.arange(groups)

    def near_first(pieces):
        return [
            lax.dynamic_index_in_dim(pieces, group_index ^ step, 0, keepdims=False)
            for step in range(groups)
        ]

    near_picks = (near_order[:, None] == jnp.arange(groups)[None, :])[:, :, None]

    split_near = send_all(split_vectors, "mp")
    split_all = jnp.sum(jnp.where(near_picks, split_near[None], 0.0), axis=1)
    count = group_width // B
    qkv_rows = qkv_master.astype(bf16).reshape(row_blocks, shard_rows, 3 * group_width)
    near = lax.ppermute(qkv_rows, "mp", [(1, 0), (3, 1), (0, 2), (2, 3)])
    inner = lax.ppermute(qkv_rows, "mp", [(1, 2), (2, 1)])
    outer = (group_index == 0) | (group_index == groups - 1)
    inner = jnp.where(outer, qkv_rows, inner)
    low_half = group_index < clips_here
    qkv_part = jnp.stack(
        [jnp.where(low_half, inner, near), jnp.where(low_half, near, inner)], axis=2
    )
    qkv_part = (
        qkv_part.reshape(row_blocks, shard_rows, part_groups, 3, group_width)
        .transpose(0, 1, 3, 2, 4)
        .reshape(row_blocks, shard_rows, 3 * part_width)
    )
    out_up = jnp.concatenate([out_master.astype(bf16), up_master.astype(bf16)], axis=0)
    out_up = send_all(out_up[None], "mp")
    down_rows = send_all(down_master.astype(bf16), "mp")
    out_rows = out_up[:, :count]
    out_rows = jnp.stack(near_first(out_rows)).reshape(-1, shard_rows, width)
    up_rows = out_up[:, count:].transpose(1, 2, 0, 3).reshape(row_blocks, shard_rows, ff)
    qkv_weight = gather(qkv_part, "dp", 1).reshape(width, 3 * part_width)
    out_weight = gather(out_rows, "dp", 1).reshape(width, width)
    up_weight = gather(up_rows, "dp", 1).reshape(width, ff)
    down_weight = gather(down_rows, "dp", 1).reshape(ff, width)
    part_bias = lax.dynamic_slice_in_dim(
        split_all[:, : 2 * group_width].reshape(groups, 2, group_width),
        my_part * part_groups,
        part_groups,
        axis=0,
    ).transpose(1, 0, 2).reshape(2, part_width)
    up_bias = split_near[:, 2 * group_width :].reshape(ff)

    tokens = inputs.transpose(1, 0, 2).astype(f32)
    normed = layer_norm(tokens, norm_gains[0], shift_vectors[0]).astype(bf16)
    normed_clip = exchange(jnp.repeat(normed, parts, axis=0), "mp").reshape(seq_len, width)
    proj_bias = jnp.concatenate([part_bias[0], jnp.zeros_like(part_bias[0]), part_bias[1]])
    proj = (dot(normed_clip, qkv_weight) + proj_bias).astype(bf16)
    attended_parts, log_parts, received = [], [], []
    for call in range(calls):
        attended_call, logs_call = attend_forward(
            proj, valid, call * call_pairs, call_pairs, row_block
        )
        attended_parts.append(attended_call)
        log_parts.append(logs_call)
        received.append(exchange(attended_call.reshape(groups, local_rows, call_width), "mp"))
    attended = jnp.stack(
        [
            jnp.concatenate(
                [
                    received[call][clip * parts + part]
                    for part in range(parts)
                    for call in range(calls)
                ],
                axis=1,
            )
            for clip in range(clips_here)
        ]
    ).reshape(tokens_here, width)
    tokens = tokens.reshape(tokens_here, width)
    hidden = tokens + dot(attended, out_weight) + shift_vectors[1]
    normed_two = layer_norm(hidden, norm_gains[1], shift_vectors[2]).astype(bf16)
    active, slope = feed_up(normed_two, up_weight, up_bias.reshape(1, ff))
    final = hidden + dot(active, down_weight) + shift_vectors[3]
    output = final.astype(bf16).reshape(clips_here, local_rows, width).transpose(1, 0, 2)

    target = teacher.transpose(1, 0, 2).reshape(tokens_here, width).astype(f32)
    grad_final = jnp.where(row_valid.reshape(tokens_here, 1), final - target, 0.0)
    grad_final_low = grad_final.astype(bf16)
    grad_down = dot(active, grad_final_low, TN).astype(bf16)
    grad_final_low, grad_down = lax.optimization_barrier((grad_final_low, grad_down))
    grad_active = dot(grad_final_low, down_weight, NT)
    grad_upper = (grad_active * slope).astype(bf16)
    grad_normed_two = dot(grad_upper, up_weight, NT)
    _, norm_two_pull = jax.vjp(layer_norm, hidden, norm_gains[1], shift_vectors[2])
    hidden_part, grad_gain_two, grad_shift_two = norm_two_pull(grad_normed_two)
    grad_hidden = grad_final + hidden_part
    grad_hidden_low = grad_hidden.astype(bf16)
    grad_attended = dot(grad_hidden_low, out_weight, NT).astype(bf16)
    by_clip_grad = grad_attended.reshape(clips_here, local_rows, width)
    outgoing_grad = [
        jnp.stack(
            [
                by_clip_grad[clip, :, at : at + call_width]
                for clip in range(clips_here)
                for at in range(call * call_width, width, part_width)
            ]
        )
        for call in range(calls)
    ]
    grad_parts = [
        exchange(outgoing_grad[call], "mp").reshape(seq_len, call_width) for call in range(calls)
    ]

    grad_out = dot(attended, grad_hidden_low, TN).astype(bf16)
    grad_up = dot(normed_two, grad_upper, TN).astype(bf16)
    grad_parts[0], grad_out, grad_up = lax.optimization_barrier((grad_parts[0], grad_out, grad_up))

    grad_down = scatter(grad_down.reshape(ff // B, B, width))
    grad_up = scatter(grad_up.reshape(row_blocks, B, ff))
    early = jnp.concatenate(
        [
            jnp.sum(grad_hidden, axis=0),
            grad_gain_two,
            grad_shift_two,
            jnp.sum(grad_final, axis=0),
            jnp.sum(
                jnp.where(near_picks, jnp.sum(grad_upper, axis=0, dtype=f32).reshape(1, groups, -1), 0.0),
                axis=1,
            ).reshape(ff),
        ]
    )
    down_shard = sum_pieces(grad_down.reshape(groups, -1, shard_rows, width), "mp")
    up_sent = grad_up.reshape(row_blocks, shard_rows, groups, group_ff).transpose(2, 0, 1, 3)
    up_shard = sum_pieces(up_sent, "mp")

    pieces = []
    for call in range(calls):
        pieces.append(
            attend_backward(
                proj,
                grad_parts[call],
                attended_parts[call],
                log_parts[call],
                valid,
                call * call_pairs,
                call_pairs,
                row_block,
            )
        )
    grad_proj = jnp.concatenate([piece[kind] for kind in range(3) for piece in pieces], axis=1)
    grad_qkv = dot(normed_clip, grad_proj, TN).astype(bf16)
    grad_proj, grad_qkv = lax.optimization_barrier((grad_proj, grad_qkv))
    last_grads = jnp.concatenate(
        [grad_qkv.reshape(row_blocks, B, 3 * part_width), grad_out.reshape(width // B, B, width)],
        axis=2,
    )
    last_grads = scatter(last_grads)
    grad_qkv, grad_out = last_grads[:, :, : 3 * part_width], last_grads[:, :, 3 * part_width :]
    out_shard = sum_pieces(near_first(grad_out.reshape(groups, -1, shard_rows, width)), "mp")
    grad_normed_part = dot(grad_proj, qkv_weight, NT).astype(bf16)
    pieces = near_first(grad_normed_part.reshape(groups, local_rows, width))
    passed = send_steps(pieces, "mp")

    first_group, second_group = [
        grad_qkv.reshape(row_blocks, shard_rows, 3, part_groups, group_width)[:, :, :, at].reshape(
            row_blocks, shard_rows, 3 * group_width
        )
        for at in range(part_groups)
    ]
    near_sent = jnp.where(low_half, second_group, first_group)
    inner_sent = jnp.where(low_half, first_group, second_group)
    near_got = lax.ppermute(near_sent, "mp", [(0, 1), (1, 3), (2, 0), (3, 2)])
    inner_got = lax.ppermute(inner_sent, "mp", [(1, 2), (2, 1)])
    qkv_shard = near_got.astype(f32) + jnp.where(outer, inner_sent, inner_got).astype(f32)
    qkv_shard = qkv_shard.reshape(row_blocks, shard_rows, 3, group_width)

    grad_blocks = jnp.concatenate(
        [
            qkv_shard.reshape(row_blocks, shard_rows, 3, group_width // B, B)
            .transpose(0, 2, 3, 1, 4)
            .reshape(-1, shard_rows, B),
            out_shard.reshape(group_width // B, shard_rows, row_blocks, B)
            .transpose(0, 2, 1, 3)
            .reshape(-1, shard_rows, B),
            up_shard.reshape(row_blocks, shard_rows, group_ff // B, B)
            .transpose(0, 2, 1, 3)
            .reshape(-1, shard_rows, B),
            down_shard.reshape(group_ff // B, shard_rows, row_blocks, B)
            .transpose(0, 2, 1, 3)
            .reshape(-1, shard_rows, B),
        ],
        axis=0,
    ).astype(bf16)
    cap_count = bases.shape[0]
    block_ids = jnp.arange(owners.shape[0])
    same_owner = owners[:, None] == owners[None, :]
    earlier = block_ids[None, :] < block_ids[:, None]
    slot_pos = jnp.sum((same_owner & earlier).astype(jnp.int32), axis=1)
    select = (
        (slot_pos[None, None, :] == jnp.arange(cap_count)[:, None, None])
        & (owners[None, None, :] == jnp.arange(shard_count)[None, :, None])
    ).astype(bf16)
    outgoing = jnp.einsum("cjk,krb->cjrb", select, grad_blocks, preferred_element_type=bf16)
    sources = jnp.stack(passed).reshape(clips_here, parts, local_rows, width)
    by_clip = jnp.sum(sources.astype(f32), axis=1)
    grad_normed = jnp.where(my_clip == 0, by_clip, by_clip[::-1]).reshape(tokens_here, width)
    _, norm_one_pull = jax.vjp(layer_norm, tokens, norm_gains[0], shift_vectors[0])
    tokens_part, grad_gain_one, grad_shift_one = norm_one_pull(grad_normed)
    input_grad = (
        (grad_hidden + tokens_part).reshape(clips_here, local_rows, width).transpose(1, 0, 2)
    )
    part_sums = jnp.sum(grad_proj, axis=0, dtype=f32).reshape(3, part_width)
    placed_sums = jnp.where(
        jnp.arange(parts)[:, None, None] == my_part, part_sums[None, ::2], 0.0
    )
    bias_rows = placed_sums.transpose(1, 0, 2).reshape(2, width)
    late = jnp.concatenate([grad_gain_one[None], grad_shift_one[None], bias_rows])
    sums = sum_everywhere(jnp.concatenate([late, early.reshape(-1, width)]))
    late_total, early_total = sums[:4], sums[4:]
    plain_total = jnp.concatenate([late_total[:2], early_total[:4]])
    split_grad = jnp.concatenate(
        [
            late_total[2].reshape(groups, group_width),
            late_total[3].reshape(groups, group_width),
            early_total[4:].reshape(groups, group_ff),
        ],
        axis=1,
    )
    split_total = lax.dynamic_slice_in_dim(split_grad, group_index, 1, axis=0)

    incoming = lax.all_to_all(outgoing, "dp", split_axis=1, concat_axis=1, tiled=True)
    incoming = (
        incoming.astype(f32)
        .reshape(cap_count, B, B)
    )
    slot_used = jnp.any(
        (owners[None, :] == shard_index) & (slot_pos[None, :] == jnp.arange(cap_count)[:, None]),
        axis=1,
    )
    old_first = first_moments[:, 0]
    old_second = second_moments[:, 0]
    new_first, new_second, update = rotate_adam(
        incoming, bases[:, 0, 0], bases[:, 0, 1], old_first, old_second
    )
    first_new = jnp.where(slot_used[:, None, None], new_first, old_first)[:, None]
    second_new = jnp.where(slot_used[:, None, None], new_second, old_second)[:, None]
    returned = lax.all_to_all(
        update.reshape(cap_count, shard_count, shard_rows, B).astype(bf16),
        "dp",
        split_axis=1,
        concat_axis=1,
        tiled=True,
    )
    picked = jnp.take(
        returned.reshape(cap_count * shard_count, shard_rows, B),
        slot_pos * shard_count + owners,
        axis=0,
    ).astype(f32)
    count_qkv = row_blocks * 3 * (group_width // B)
    count_out = group_width // B * row_blocks
    count_up = row_blocks * (group_ff // B)
    qkv_update = (
        picked[:count_qkv]
        .reshape(row_blocks, 3, group_width // B, shard_rows, B)
        .transpose(0, 3, 1, 2, 4)
        .reshape(row_blocks, shard_rows, 3, group_width)
    )
    out_update = (
        picked[count_qkv : count_qkv + count_out]
        .reshape(group_width // B, row_blocks, shard_rows, B)
        .transpose(0, 2, 1, 3)
        .reshape(group_width // B, shard_rows, width)
    )
    up_update = (
        picked[count_qkv + count_out : count_qkv + count_out + count_up]
        .reshape(row_blocks, group_ff // B, shard_rows, B)
        .transpose(0, 2, 1, 3)
        .reshape(row_blocks, shard_rows, group_ff)
    )
    down_update = (
        picked[count_qkv + count_out + count_up :]
        .reshape(group_ff // B, row_blocks, shard_rows, B)
        .transpose(0, 2, 1, 3)
        .reshape(group_ff // B, shard_rows, width)
    )
    qkv_new = qkv_master - rate_qkv * qkv_update
    out_new = out_master - rate_out * out_update
    up_new = up_master - rate_up * up_update
    down_new = down_master - rate_down * down_update
    plain_param = jnp.stack(
        [
            norm_gains[0],
            shift_vectors[0],
            shift_vectors[1],
            norm_gains[1],
            shift_vectors[2],
            shift_vectors[3],
        ]
    )
    plain_new, plain_first_new, plain_second_new = adam_rows(
        plain_total, plain_param, plain_first, plain_second
    )
    gains_new = jnp.stack([plain_new[0], plain_new[3]])
    shifts_new = jnp.stack([plain_new[1], plain_new[2], plain_new[4], plain_new[5]])
    split_new, split_first_new, split_second_new = adam_rows(
        split_total, split_vectors, split_first, split_second
    )
    return (
        output,
        input_grad,
        qkv_new,
        out_new,
        up_new,
        down_new,
        qkv_new.astype(bf16),
        out_new.astype(bf16),
        up_new.astype(bf16),
        down_new.astype(bf16),
        gains_new,
        shifts_new,
        split_new,
        first_new,
        second_new,
        plain_first_new,
        plain_second_new,
        split_first_new,
        split_second_new,
    )


def solution(mesh):
    placed = (
        P("mp", "dp", None),
        P("mp", "dp", None),
        P("dp"),
        P(),
        P(None, "dp", None, "mp"),
        P("mp", "dp", None),
        P(None, "dp", "mp"),
        P("mp", "dp", None),
        P(),
        P(),
        P("mp", None),
        P("dp", "mp", None, None, None),
        P("dp", "mp", None, None),
        P("dp", "mp", None, None),
        P(),
        P(),
        P("mp", None),
        P("mp", None),
    )
    return jax.shard_map(
        per_device,
        mesh=mesh,
        in_specs=placed,
        out_specs=(
            P("mp", "dp", None),
            P("mp", "dp", None),
            P(None, "dp", None, "mp"),
            P("mp", "dp", None),
            P(None, "dp", "mp"),
            P("mp", "dp", None),
            P(None, "dp", None, "mp"),
            P("mp", "dp", None),
            P(None, "dp", "mp"),
            P("mp", "dp", None),
            P(),
            P(),
            P("mp", None),
            P("dp", "mp", None, None),
            P("dp", "mp", None, None),
            P(),
            P(),
            P("mp", None),
            P("mp", None),
        ),
        check_vma=False,
    )
```

```python
from functools import partial

import jax
import jax.numpy as jnp
from jax import lax
from jax.experimental import pallas as pl
from jax.experimental.pallas import tpu as pltpu
from jax.sharding import PartitionSpec as P


HD = 64
B = 128
PAIR = 2 * HD


eps_norm = 1e-06
eps_adam = 1e-08
beta_first = 0.5
beta_second = 0.6
rate_qkv = 0.016
rate_out = 0.25
rate_up = 0.016
rate_down = 0.008
rate_vector = 0.3
scale_score = 0.125

f32 = jnp.float32
bf16 = jnp.bfloat16
NT = (((1,), (1,)), ((), ()))
NN = (((1,), (0,)), ((), ()))
TN = (((0,), (0,)), ((), ()))


def dot(left, right, dims=NN):
    return lax.dot_general(left, right, dims, preferred_element_type=f32)


def layer_norm(values, scale_row, shift_row):
    average = jnp.mean(values, axis=-1, keepdims=True)
    centered = values - average
    variance = jnp.mean(centered * centered, axis=-1, keepdims=True)
    return centered * lax.rsqrt(variance + 1e-06) * scale_row + shift_row


def adam_rows(grad_rows, param_rows, first_rows, second_rows):
    scaled = grad_rows * lax.rsqrt(
        jnp.mean(grad_rows * grad_rows, axis=-1, keepdims=True) + eps_norm
    )
    new_first = beta_first * first_rows + (1.0 - beta_first) * scaled
    new_second = beta_second * second_rows + (1.0 - beta_second) * scaled * scaled
    step_rows = new_first / (jnp.sqrt(new_second) + eps_adam)
    return (param_rows - rate_vector * step_rows, new_first, new_second)


def rotate_adam(grad_blocks, left_basis, right_basis, old_first, old_second):
    high = lax.Precision.HIGH
    scaled = grad_blocks * lax.rsqrt(
        jnp.mean(grad_blocks * grad_blocks, axis=(1, 2), keepdims=True) + eps_norm
    )
    rotated = jnp.einsum("kba,kbd->kad", left_basis, scaled, precision=high)
    rotated = jnp.einsum("kad,kde->kae", rotated, right_basis, precision=high)
    new_first = beta_first * old_first + (1.0 - beta_first) * rotated
    new_second = beta_second * old_second + (1.0 - beta_second) * rotated * rotated
    step_rot = new_first / (jnp.sqrt(new_second) + eps_adam)
    update = jnp.einsum("kab,kbd->kad", left_basis, step_rot, precision=high)
    update = jnp.einsum("kad,ked->kae", update, right_basis, precision=high)
    return (new_first, new_second, update)


def lane_index(rows):
    return lax.broadcasted_iota(jnp.int32, (rows, PAIR), 1)


def own_lanes(lane, head):
    return lane < HD if head == 0 else lane >= HD


def key_operands(keys, first_row, valid):
    rows = keys.shape[0]
    lane = lane_index(rows)
    row = lax.broadcasted_iota(jnp.int32, (rows, PAIR), 0) + first_row
    wide = keys.astype(f32)
    padding = jnp.where(row >= valid, -1e30, 0.0)
    operands = []
    for head in range(2):
        base = HD * (1 - head)
        other = jnp.where(lane < base + 3, 1.0, jnp.where(lane == base + 3, padding, 0.0))
        operands.append(jnp.where(own_lanes(lane, head), wide, other).astype(bf16))
    return operands


def forward_kernel(chunk, valid_ref, q_ref, k_ref, v_ref, out_ref, log_ref, key_ref, score_ref):
    tokens = q_ref.shape[0]
    lane = lane_index(tokens)
    queries = q_ref[...].astype(f32) * scale_score
    ones = jnp.ones((16, chunk), f32)
    starts = range(0, tokens, chunk)
    outputs, logs = [], []
    for head, operand in enumerate(key_operands(k_ref[...], 0, valid_ref[0])):
        mark = jnp.where(lane == HD * (1 - head) + 3, 1.0, 0.0)
        query = jnp.where(own_lanes(lane, head), queries, mark).astype(bf16)
        key_ref[head] = operand
        top = None
        for at in starts:
            scores = dot(key_ref[head, at : at + chunk], query, NT)
            score_ref[head, at : at + chunk] = scores
            peak = jnp.max(scores, axis=0, keepdims=True)
            top = peak if top is None else jnp.maximum(top, peak)
        total = None
        for at in starts:
            turned = jnp.transpose(v_ref[at : at + chunk].astype(f32))
            values = jnp.concatenate([turned[HD * head : HD * head + HD], ones], axis=0)
            weight = jnp.exp(score_ref[head, at : at + chunk] - top).astype(bf16)
            term = dot(values.astype(bf16), weight)
            total = term if total is None else total + term
        weight_sum = total[HD : HD + 1]
        outputs.append(total[:HD] / weight_sum)
        logs.append(-(top + jnp.log(weight_sum)))
    out_ref[...] = jnp.transpose(jnp.concatenate(outputs, axis=0)).astype(bf16)
    column = jnp.ones((HD, 1), f32)
    log_ref[...] = jnp.transpose(jnp.concatenate([column * logs[1], column * logs[0]], axis=0))


def attend_forward(proj, valid, first_pair, pairs, chunk):
    tokens = proj.shape[0]
    per_part = proj.shape[1] // 3 // PAIR

    def pair_spec(at):
        return pl.BlockSpec((tokens, PAIR), lambda pair: (0, at + pair))

    return pl.pallas_call(
        partial(forward_kernel, chunk),
        grid=(pairs,),
        in_specs=[
            pl.BlockSpec(memory_space=pltpu.SMEM),
            pair_spec(first_pair),
            pair_spec(per_part + first_pair),
            pair_spec(2 * per_part + first_pair),
        ],
        out_specs=[pair_spec(0), pair_spec(0)],
        out_shape=[
            jax.ShapeDtypeStruct((tokens, pairs * PAIR), bf16),
            jax.ShapeDtypeStruct((tokens, pairs * PAIR), f32),
        ],
        scratch_shapes=[
            pltpu.VMEM((2, tokens, PAIR), bf16),
            pltpu.VMEM((2, tokens, tokens), f32),
        ],
        compiler_params=pltpu.CompilerParams(vmem_limit_bytes=58 * 2**20),
        cost_estimate=pl.CostEstimate(
            flops=16 * pairs * tokens * tokens * PAIR,
            bytes_accessed=pairs * tokens * PAIR * 12,
            transcendentals=pairs * 2 * tokens * tokens,
        ),
    )(valid, proj, proj, proj)


def backward_kernel(
    chunk,
    valid_ref,
    q_ref,
    k_ref,
    v_ref,
    grad_ref,
    out_ref,
    log_ref,
    dq_ref,
    dk_ref,
    dv_ref,
    query_ref,
    cot_ref,
    turned_ref,
):
    tokens = q_ref.shape[0]
    lane = lane_index(tokens)
    queries = q_ref[...].astype(f32) * scale_score
    logs = log_ref[...]
    log_high = logs.astype(bf16).astype(f32)
    log_rest = logs - log_high
    log_middle = log_rest.astype(bf16).astype(f32)
    log_low = log_rest - log_middle
    grad = grad_ref[...].astype(f32)
    product = grad * out_ref[...].astype(f32)
    product_high = product.astype(bf16)
    product_low = (product - product_high.astype(f32)).astype(bf16)
    source = lax.broadcasted_iota(jnp.int32, (PAIR, PAIR), 0)
    target = lax.broadcasted_iota(jnp.int32, (PAIR, PAIR), 1)
    place = jnp.where((source < HD) != (target < HD), -1.0, 0.0).astype(bf16)
    delta = dot(product_high, place) + dot(product_low, place)
    delta_high = delta.astype(bf16).astype(f32)
    delta_low = delta - delta_high
    for head in range(2):
        base = HD * (1 - head)
        mine = own_lanes(lane, head)
        mark = jnp.where(lane == base + 3, 1.0, 0.0)
        other = jnp.where(lane == base + 2, log_low, mark)
        other = jnp.where(lane == base + 1, log_middle, other)
        other = jnp.where(lane == base, log_high, other)
        query_ref[head] = jnp.where(mine, queries, other).astype(bf16)
        other = jnp.where(lane == base + 1, delta_low, 0.0)
        other = jnp.where(lane == base, delta_high, other)
        cot_ref[head] = jnp.where(mine, grad, other).astype(bf16)

    key_lane = lane_index(chunk)
    for at in range(0, tokens, chunk):
        rows = slice(at, at + chunk)
        operands = key_operands(k_ref[rows], at, valid_ref[0])
        wide_values = v_ref[rows].astype(f32)
        turned_keys = jnp.transpose(k_ref[rows].astype(f32)).astype(bf16)
        dk, dv = [], []
        for head in range(2):
            base = HD * (1 - head)
            span = slice(HD * head, HD * head + HD)
            pair_of_ones = jnp.where((key_lane == base) | (key_lane == base + 1), 1.0, 0.0)
            values = jnp.where(own_lanes(key_lane, head), wide_values, pair_of_ones).astype(bf16)
            weight = jnp.exp(dot(operands[head], query_ref[head], NT))
            slope = (weight * dot(values, cot_ref[head], NT)).astype(bf16)
            dv.append(dot(weight.astype(bf16), cot_ref[head]))
            dk.append(dot(slope, query_ref[head]))
            term = dot(turned_keys[span], slope)
            turned_ref[span] = term if at == 0 else turned_ref[span] + term
        dk_ref[rows] = jnp.where(key_lane < HD, dk[0], dk[1]).astype(bf16)
        dv_ref[rows] = jnp.where(key_lane < HD, dv[0], dv[1]).astype(bf16)
    dq_ref[...] = (jnp.transpose(turned_ref[...]) * scale_score).astype(bf16)


def attend_backward(proj, grad, attended, logs, valid, first_pair, pairs, chunk):
    tokens = proj.shape[0]
    per_part = proj.shape[1] // 3 // PAIR

    def pair_spec(at):
        return pl.BlockSpec((tokens, PAIR), lambda pair: (0, at + pair))

    return pl.pallas_call(
        partial(backward_kernel, chunk),
        grid=(pairs,),
        in_specs=[
            pl.BlockSpec(memory_space=pltpu.SMEM),
            pair_spec(first_pair),
            pair_spec(per_part + first_pair),
            pair_spec(2 * per_part + first_pair),
            pair_spec(0),
            pair_spec(0),
            pair_spec(0),
        ],
        out_specs=[pair_spec(0)] * 3,
        out_shape=[jax.ShapeDtypeStruct((tokens, pairs * PAIR), bf16)] * 3,
        scratch_shapes=[
            pltpu.VMEM((2, tokens, PAIR), bf16),
            pltpu.VMEM((2, tokens, PAIR), bf16),
            pltpu.VMEM((PAIR, tokens), f32),
        ],
        compiler_params=pltpu.CompilerParams(vmem_limit_bytes=58 * 2**20),
        cost_estimate=pl.CostEstimate(
            flops=40 * pairs * tokens * tokens * PAIR,
            bytes_accessed=pairs * tokens * PAIR * 24,
            transcendentals=pairs * 2 * tokens * tokens,
        ),
    )(valid, proj, proj, proj, grad, attended, logs)


def feed_kernel(chunk, normed_ref, weight_ref, bias_ref, active_ref, slope_ref):
    for at in range(0, normed_ref.shape[0], chunk):
        rows = slice(at, at + chunk)
        upper = dot(normed_ref[rows], weight_ref[...]) + bias_ref[...]
        below = 0.5 + 0.5 * lax.erf(upper * 0.7071067811865476)
        active_ref[rows] = (upper * below).astype(bf16)
        density = 0.3989422804014327 * jnp.exp(-0.5 * upper * upper)
        slope_ref[rows] = (below + upper * density).astype(bf16)


def feed_up(normed, weight, bias):
    tokens, width = normed.shape
    columns = 512
    by_column = pl.BlockSpec((tokens, columns), lambda step: (0, step))
    return pl.pallas_call(
        partial(feed_kernel, tokens // 7),
        grid=(weight.shape[1] // columns,),
        in_specs=[
            pl.BlockSpec((tokens, width), lambda step: (0, 0)),
            pl.BlockSpec((width, columns), lambda step: (0, step)),
            pl.BlockSpec((1, columns), lambda step: (0, step)),
        ],
        out_specs=[by_column, by_column],
        out_shape=[jax.ShapeDtypeStruct((tokens, weight.shape[1]), bf16)] * 2,
        compiler_params=pltpu.CompilerParams(vmem_limit_bytes=48 * 2**20),
        cost_estimate=pl.CostEstimate(
            flops=2 * tokens * width * weight.shape[1],
            bytes_accessed=4 * tokens * weight.shape[1] + 2 * width * weight.shape[1],
            transcendentals=2 * tokens * weight.shape[1],
        ),
    )(normed, weight, bias)


def exchange(values, axis):
    return lax.all_to_all(values, axis, split_axis=0, concat_axis=0, tiled=True)


def gather(values, axis, dimension):
    return lax.all_gather(values, axis, axis=dimension, tiled=True)


def scatter(values):
    return lax.psum_scatter(values, "dp", scatter_dimension=1, tiled=True)


def send_steps(pieces, axis):
    size = lax.axis_size(axis)
    arrived = [pieces[0]]
    for step in range(1, size):
        arrived.append(lax.ppermute(pieces[step], axis, [(i, i ^ step) for i in range(size)]))
    return arrived


def send_all(values, axis):
    size = lax.axis_size(axis)
    arrived = [values]
    for step in range(1, size):
        arrived.append(lax.ppermute(values, axis, [(i, i ^ step) for i in range(size)]))
    return jnp.concatenate(arrived, axis=0)


def sum_pieces(pieces, axis):
    total = None
    for piece in send_steps(pieces, axis):
        total = piece.astype(f32) if total is None else total + piece.astype(f32)
    return total


def sum_everywhere(values):
    for axis in ("dp", "mp"):
        size = lax.axis_size(axis)
        bit = 1
        while bit < size:
            other = lax.ppermute(values, axis, [(i, i ^ bit) for i in range(size)])
            values = values + other
            bit *= 2
    return values


def per_device(
    inputs,
    teacher,
    clip_tokens,
    owners,
    qkv_master,
    out_master,
    up_master,
    down_master,
    norm_gains,
    shift_vectors,
    split_vectors,
    bases,
    first_moments,
    second_moments,
    plain_first,
    plain_second,
    split_first,
    split_second,
):
    local_rows, clips_here, width = inputs.shape
    groups = lax.axis_size("mp")
    group_index = lax.axis_index("mp")
    shard_count = lax.axis_size("dp")
    shard_index = lax.axis_index("dp")
    seq_len = local_rows * groups
    row_blocks, shard_rows, _, group_width = qkv_master.shape
    group_ff = up_master.shape[2]
    ff = group_ff * groups
    tokens_here = clips_here * local_rows
    assert groups == 4 and clips_here == 2
    parts = groups // clips_here
    part_groups = groups // parts
    part_width = part_groups * group_width
    my_clip = group_index // parts
    my_part = group_index % parts
    pairs = part_width // PAIR
    calls = 2
    call_pairs = pairs // calls
    call_width = call_pairs * PAIR
    row_block = seq_len // 7

    positions = group_index * local_rows + jnp.arange(local_rows)
    row_valid = positions[None, :] < clip_tokens[:, None]
    valid = lax.dynamic_slice(clip_tokens, (my_clip,), (1,))
    near_order = group_index ^ jnp.arange(groups)

    def near_first(pieces):
        return [
            lax.dynamic_index_in_dim(pieces, group_index ^ step, 0, keepdims=False)
            for step in range(groups)
        ]

    near_picks = (near_order[:, None] == jnp.arange(groups)[None, :])[:, :, None]

    split_near = send_all(split_vectors, "mp")
    split_all = jnp.sum(jnp.where(near_picks, split_near[None], 0.0), axis=1)
    count = group_width // B
    qkv_rows = qkv_master.astype(bf16).reshape(row_blocks, shard_rows, 3 * group_width)
    near = lax.ppermute(qkv_rows, "mp", [(1, 0), (3, 1), (0, 2), (2, 3)])
    inner = lax.ppermute(qkv_rows, "mp", [(1, 2), (2, 1)])
    outer = (group_index == 0) | (group_index == groups - 1)
    inner = jnp.where(outer, qkv_rows, inner)
    low_half = group_index < clips_here
    qkv_part = jnp.stack(
        [jnp.where(low_half, inner, near), jnp.where(low_half, near, inner)], axis=2
    )
    qkv_part = (
        qkv_part.reshape(row_blocks, shard_rows, part_groups, 3, group_width)
        .transpose(0, 1, 3, 2, 4)
        .reshape(row_blocks, shard_rows, 3 * part_width)
    )
    out_up = jnp.concatenate([out_master.astype(bf16), up_master.astype(bf16)], axis=0)
    out_up = send_all(out_up[None], "mp")
    down_rows = send_all(down_master.astype(bf16), "mp")
    out_rows = out_up[:, :count]
    out_rows = jnp.stack(near_first(out_rows)).reshape(-1, shard_rows, width)
    up_rows = out_up[:, count:].transpose(1, 2, 0, 3).reshape(row_blocks, shard_rows, ff)
    qkv_weight = gather(qkv_part, "dp", 1).reshape(width, 3 * part_width)
    out_weight = gather(out_rows, "dp", 1).reshape(width, width)
    up_weight = gather(up_rows, "dp", 1).reshape(width, ff)
    down_weight = gather(down_rows, "dp", 1).reshape(ff, width)
    part_bias = lax.dynamic_slice_in_dim(
        split_all[:, : 2 * group_width].reshape(groups, 2, group_width),
        my_part * part_groups,
        part_groups,
        axis=0,
    ).transpose(1, 0, 2).reshape(2, part_width)
    up_bias = split_near[:, 2 * group_width :].reshape(ff)

    tokens = inputs.transpose(1, 0, 2).astype(f32)
    normed = layer_norm(tokens, norm_gains[0], shift_vectors[0]).astype(bf16)
    normed_clip = exchange(jnp.repeat(normed, parts, axis=0), "mp").reshape(seq_len, width)
    proj_bias = jnp.concatenate([part_bias[0], jnp.zeros_like(part_bias[0]), part_bias[1]])
    proj = (dot(normed_clip, qkv_weight) + proj_bias).astype(bf16)
    attended_parts, log_parts, received = [], [], []
    for call in range(calls):
        attended_call, logs_call = attend_forward(
            proj, valid, call * call_pairs, call_pairs, row_block
        )
        attended_parts.append(attended_call)
        log_parts.append(logs_call)
        received.append(exchange(attended_call.reshape(groups, local_rows, call_width), "mp"))
    attended = jnp.stack(
        [
            jnp.concatenate(
                [
                    received[call][clip * parts + part]
                    for part in range(parts)
                    for call in range(calls)
                ],
                axis=1,
            )
            for clip in range(clips_here)
        ]
    ).reshape(tokens_here, width)
    tokens = tokens.reshape(tokens_here, width)
    hidden = tokens + dot(attended, out_weight) + shift_vectors[1]
    normed_two = layer_norm(hidden, norm_gains[1], shift_vectors[2]).astype(bf16)
    active, slope = feed_up(normed_two, up_weight, up_bias.reshape(1, ff))
    final = hidden + dot(active, down_weight) + shift_vectors[3]
    output = final.astype(bf16).reshape(clips_here, local_rows, width).transpose(1, 0, 2)

    target = teacher.transpose(1, 0, 2).reshape(tokens_here, width).astype(f32)
    grad_final = jnp.where(row_valid.reshape(tokens_here, 1), final - target, 0.0)
    grad_final_low = grad_final.astype(bf16)
    grad_down = dot(active, grad_final_low, TN).astype(bf16)
    grad_final_low, grad_down = lax.optimization_barrier((grad_final_low, grad_down))
    grad_active = dot(grad_final_low, down_weight, NT)
    grad_upper = (grad_active * slope).astype(bf16)
    grad_normed_two = dot(grad_upper, up_weight, NT)
    _, norm_two_pull = jax.vjp(layer_norm, hidden, norm_gains[1], shift_vectors[2])
    hidden_part, grad_gain_two, grad_shift_two = norm_two_pull(grad_normed_two)
    grad_hidden = grad_final + hidden_part
    grad_hidden_low = grad_hidden.astype(bf16)
    grad_attended = dot(grad_hidden_low, out_weight, NT).astype(bf16)
    by_clip_grad = grad_attended.reshape(clips_here, local_rows, width)
    outgoing_grad = [
        jnp.stack(
            [
                by_clip_grad[clip, :, at : at + call_width]
                for clip in range(clips_here)
                for at in range(call * call_width, width, part_width)
            ]
        )
        for call in range(calls)
    ]
    grad_parts = [
        exchange(outgoing_grad[call], "mp").reshape(seq_len, call_width) for call in range(calls)
    ]

    grad_out = dot(attended, grad_hidden_low, TN).astype(bf16)
    grad_up = dot(normed_two, grad_upper, TN).astype(bf16)
    grad_parts[0], grad_out, grad_up = lax.optimization_barrier((grad_parts[0], grad_out, grad_up))

    grad_down = scatter(grad_down.reshape(ff // B, B, width))
    grad_up = scatter(grad_up.reshape(row_blocks, B, ff))
    early = jnp.concatenate(
        [
            jnp.sum(grad_hidden, axis=0),
            grad_gain_two,
            grad_shift_two,
            jnp.sum(grad_final, axis=0),
            jnp.sum(
                jnp.where(near_picks, jnp.sum(grad_upper, axis=0, dtype=f32).reshape(1, groups, -1), 0.0),
                axis=1,
            ).reshape(ff),
        ]
    )
    down_shard = sum_pieces(grad_down.reshape(groups, -1, shard_rows, width), "mp")
    up_sent = grad_up.reshape(row_blocks, shard_rows, groups, group_ff).transpose(2, 0, 1, 3)
    up_shard = sum_pieces(up_sent, "mp")

    pieces = []
    for call in range(calls):
        pieces.append(
            attend_backward(
                proj,
                grad_parts[call],
                attended_parts[call],
                log_parts[call],
                valid,
                call * call_pairs,
                call_pairs,
                row_block,
            )
        )
    grad_proj = jnp.concatenate([piece[kind] for kind in range(3) for piece in pieces], axis=1)
    grad_qkv = dot(normed_clip, grad_proj, TN).astype(bf16)
    grad_proj, grad_qkv = lax.optimization_barrier((grad_proj, grad_qkv))
    last_grads = jnp.concatenate(
        [grad_qkv.reshape(row_blocks, B, 3 * part_width), grad_out.reshape(width // B, B, width)],
        axis=2,
    )
    last_grads = scatter(last_grads)
    grad_qkv, grad_out = last_grads[:, :, : 3 * part_width], last_grads[:, :, 3 * part_width :]
    out_shard = sum_pieces(near_first(grad_out.reshape(groups, -1, shard_rows, width)), "mp")
    grad_normed_part = dot(grad_proj, qkv_weight, NT).astype(bf16)
    pieces = near_first(grad_normed_part.reshape(groups, local_rows, width))
    passed = send_steps(pieces, "mp")

    first_group, second_group = [
        grad_qkv.reshape(row_blocks, shard_rows, 3, part_groups, group_width)[:, :, :, at].reshape(
            row_blocks, shard_rows, 3 * group_width
        )
        for at in range(part_groups)
    ]
    near_sent = jnp.where(low_half, second_group, first_group)
    inner_sent = jnp.where(low_half, first_group, second_group)
    near_got = lax.ppermute(near_sent, "mp", [(0, 1), (1, 3), (2, 0), (3, 2)])
    inner_got = lax.ppermute(inner_sent, "mp", [(1, 2), (2, 1)])
    qkv_shard = near_got.astype(f32) + jnp.where(outer, inner_sent, inner_got).astype(f32)
    qkv_shard = qkv_shard.reshape(row_blocks, shard_rows, 3, group_width)

    grad_blocks = jnp.concatenate(
        [
            qkv_shard.reshape(row_blocks, shard_rows, 3, group_width // B, B)
            .transpose(0, 2, 3, 1, 4)
            .reshape(-1, shard_rows, B),
            out_shard.reshape(group_width // B, shard_rows, row_blocks, B)
            .transpose(0, 2, 1, 3)
            .reshape(-1, shard_rows, B),
            up_shard.reshape(row_blocks, shard_rows, group_ff // B, B)
            .transpose(0, 2, 1, 3)
            .reshape(-1, shard_rows, B),
            down_shard.reshape(group_ff // B, shard_rows, row_blocks, B)
            .transpose(0, 2, 1, 3)
            .reshape(-1, shard_rows, B),
        ],
        axis=0,
    ).astype(bf16)
    cap_count = bases.shape[0]
    block_ids = jnp.arange(owners.shape[0])
    same_owner = owners[:, None] == owners[None, :]
    earlier = block_ids[None, :] < block_ids[:, None]
    slot_pos = jnp.sum((same_owner & earlier).astype(jnp.int32), axis=1)
    select = (
        (slot_pos[None, None, :] == jnp.arange(cap_count)[:, None, None])
        & (owners[None, None, :] == jnp.arange(shard_count)[None, :, None])
    ).astype(bf16)
    outgoing = jnp.einsum("cjk,krb->cjrb", select, grad_blocks, preferred_element_type=bf16)
    sources = jnp.stack(passed).reshape(clips_here, parts, local_rows, width)
    by_clip = jnp.sum(sources.astype(f32), axis=1)
    grad_normed = jnp.where(my_clip == 0, by_clip, by_clip[::-1]).reshape(tokens_here, width)
    _, norm_one_pull = jax.vjp(layer_norm, tokens, norm_gains[0], shift_vectors[0])
    tokens_part, grad_gain_one, grad_shift_one = norm_one_pull(grad_normed)
    input_grad = (
        (grad_hidden + tokens_part).reshape(clips_here, local_rows, width).transpose(1, 0, 2)
    )
    part_sums = jnp.sum(grad_proj, axis=0, dtype=f32).reshape(3, part_width)
    placed_sums = jnp.where(
        jnp.arange(parts)[:, None, None] == my_part, part_sums[None, ::2], 0.0
    )
    bias_rows = placed_sums.transpose(1, 0, 2).reshape(2, width)
    late = jnp.concatenate([grad_gain_one[None], grad_shift_one[None], bias_rows])
    sums = sum_everywhere(jnp.concatenate([late, early.reshape(-1, width)]))
    late_total, early_total = sums[:4], sums[4:]
    plain_total = jnp.concatenate([late_total[:2], early_total[:4]])
    split_grad = jnp.concatenate(
        [
            late_total[2].reshape(groups, group_width),
            late_total[3].reshape(groups, group_width),
            early_total[4:].reshape(groups, group_ff),
        ],
        axis=1,
    )
    split_total = lax.dynamic_slice_in_dim(split_grad, group_index, 1, axis=0)

    incoming = lax.all_to_all(outgoing, "dp", split_axis=1, concat_axis=1, tiled=True)
    incoming = (
        incoming.astype(f32)
        .reshape(cap_count, B, B)
    )
    slot_used = jnp.any(
        (owners[None, :] == shard_index) & (slot_pos[None, :] == jnp.arange(cap_count)[:, None]),
        axis=1,
    )
    old_first = first_moments[:, 0]
    old_second = second_moments[:, 0]
    new_first, new_second, update = rotate_adam(
        incoming, bases[:, 0, 0], bases[:, 0, 1], old_first, old_second
    )
    first_new = jnp.where(slot_used[:, None, None], new_first, old_first)[:, None]
    second_new = jnp.where(slot_used[:, None, None], new_second, old_second)[:, None]
    returned = lax.all_to_all(
        update.reshape(cap_count, shard_count, shard_rows, B).astype(bf16),
        "dp",
        split_axis=1,
        concat_axis=1,
        tiled=True,
    )
    picked = jnp.take(
        returned.reshape(cap_count * shard_count, shard_rows, B),
        slot_pos * shard_count + owners,
        axis=0,
    ).astype(f32)
    count_qkv = row_blocks * 3 * (group_width // B)
    count_out = group_width // B * row_blocks
    count_up = row_blocks * (group_ff // B)
    qkv_update = (
        picked[:count_qkv]
        .reshape(row_blocks, 3, group_width // B, shard_rows, B)
        .transpose(0, 3, 1, 2, 4)
        .reshape(row_blocks, shard_rows, 3, group_width)
    )
    out_update = (
        picked[count_qkv : count_qkv + count_out]
        .reshape(group_width // B, row_blocks, shard_rows, B)
        .transpose(0, 2, 1, 3)
        .reshape(group_width // B, shard_rows, width)
    )
    up_update = (
        picked[count_qkv + count_out : count_qkv + count_out + count_up]
        .reshape(row_blocks, group_ff // B, shard_rows, B)
        .transpose(0, 2, 1, 3)
        .reshape(row_blocks, shard_rows, group_ff)
    )
    down_update = (
        picked[count_qkv + count_out + count_up :]
        .reshape(group_ff // B, row_blocks, shard_rows, B)
        .transpose(0, 2, 1, 3)
        .reshape(group_ff // B, shard_rows, width)
    )
    qkv_new = qkv_master - rate_qkv * qkv_update
    out_new = out_master - rate_out * out_update
    up_new = up_master - rate_up * up_update
    down_new = down_master - rate_down * down_update
    plain_param = jnp.stack(
        [
            norm_gains[0],
            shift_vectors[0],
            shift_vectors[1],
            norm_gains[1],
            shift_vectors[2],
            shift_vectors[3],
        ]
    )
    plain_new, plain_first_new, plain_second_new = adam_rows(
        plain_total, plain_param, plain_first, plain_second
    )
    gains_new = jnp.stack([plain_new[0], plain_new[3]])
    shifts_new = jnp.stack([plain_new[1], plain_new[2], plain_new[4], plain_new[5]])
    split_new, split_first_new, split_second_new = adam_rows(
        split_total, split_vectors, split_first, split_second
    )
    return (
        output,
        input_grad,
        qkv_new,
        out_new,
        up_new,
        down_new,
        qkv_new.astype(bf16),
        out_new.astype(bf16),
        up_new.astype(bf16),
        down_new.astype(bf16),
        gains_new,
        shifts_new,
        split_new,
        first_new,
        second_new,
        plain_first_new,
        plain_second_new,
        split_first_new,
        split_second_new,
    )


def solution(mesh):
    placed = (
        P("mp", "dp", None),
        P("mp", "dp", None),
        P("dp"),
        P(),
        P(None, "dp", None, "mp"),
        P("mp", "dp", None),
        P(None, "dp", "mp"),
        P("mp", "dp", None),
        P(),
        P(),
        P("mp", None),
        P("dp", "mp", None, None, None),
        P("dp", "mp", None, None),
        P("dp", "mp", None, None),
        P(),
        P(),
        P("mp", None),
        P("mp", None),
    )
    return jax.shard_map(
        per_device,
        mesh=mesh,
        in_specs=placed,
        out_specs=(
            P("mp", "dp", None),
            P("mp", "dp", None),
            P(None, "dp", None, "mp"),
            P("mp", "dp", None),
            P(None, "dp", "mp"),
            P("mp", "dp", None),
            P(None, "dp", None, "mp"),
            P("mp", "dp", None),
            P(None, "dp", "mp"),
            P("mp", "dp", None),
            P(),
            P(),
            P("mp", None),
            P("dp", "mp", None, None),
            P("dp", "mp", None, None),
            P(),
            P(),
            P("mp", None),
            P("mp", None),
        ),
        check_vma=False,
    )
```
